256 devices in a mesh: lat: 4 (over z_hi), lon: 64 (over x, y, z_lo, core).
Axes of the slice: x: 4, y: 4, z: 8 (z_hi: 4, z_lo: 2; z = z_hi * 2 + z_lo), core: 2. Of those that a mesh axis runs over, the one named last changes fastest.
Arguments:
- poleward_flow: float32 [10, 4, 256, 8192], P(None, None, 'lat', 'lon'), may hold values from -16 to 16
- potential_warmth: float32 [10, 4, 256, 8192], P(None, None, 'lat', 'lon'), may hold values from -16 to 16
- water_profile_flag: int32 [256, 8192], P('lat', 'lon'), may hold values from 0 to 1
- floor_count: int32 [256, 8192], P('lat', 'lon'), may hold values from 0 to 4, as said below
- catchment_label_for_site: int32 [256, 8192], P('lat', 'lon'), may hold values from 0 to 9
Outputs:
- eddy_temp: float32 [4, 256, 8192], P(None, 'lat', 'lon')
- transport: float32 [4, 10, 4, 256], P(None, None, None, ('lat', 'lon'))
The draws below stay inside these ranges and needn't reach their ends.
Inputs may be any that keep to these rules, and one draw needn't show every extreme that they name: `floor_count`: land rows of zeros occur at some latitudes; elsewhere columns have 1 to 4 wet levels.
All inputs are finite; a program needn't handle non-finite values.
Results may differ from the reference program's by a relative error of at most 0.0003.
Values sent between devices are 32-bit elements; how exact they have to be, the bound alone decides.
A program may use at most 64 MiB of HBM per device.

```python
import math
import jax
import jax.numpy as jnp
from jax import lax

SNAPSHOT_TIMES = 10
LAYERS = 4
BASINS = 10
MERIDIAN_POINTS = 256
LONGITUDE_SLOTS = 8192


def ocean_fields(key):
    generator_keys = jax.random.split(jax.random.fold_in(key, 11), 10)
    along_latitude_flow = jax.random.normal(generator_keys[0], (1, LAYERS, MERIDIAN_POINTS, 1), jnp.float32)
    along_latitude_warmth = jax.random.normal(generator_keys[1], (1, LAYERS, MERIDIAN_POINTS, 1), jnp.float32)
    residual_transport_term = jax.random.normal(generator_keys[2], (SNAPSHOT_TIMES, LAYERS, MERIDIAN_POINTS, 1), jnp.float32)
    thermal_deviate = 0.6 * residual_transport_term + 0.8 * jax.random.normal(generator_keys[3], (SNAPSHOT_TIMES, LAYERS, MERIDIAN_POINTS, 1), jnp.float32)
    steady_share = jax.random.normal(generator_keys[4], (1, LAYERS, MERIDIAN_POINTS, LONGITUDE_SLOTS), jnp.float32)
    steady_warmth = jax.random.normal(generator_keys[5], (1, LAYERS, MERIDIAN_POINTS, LONGITUDE_SLOTS), jnp.float32)
    speed_residual = jax.random.normal(generator_keys[6], (SNAPSHOT_TIMES, LAYERS, MERIDIAN_POINTS, LONGITUDE_SLOTS), jnp.float32)
    thermal_residual = jax.random.normal(generator_keys[7], (SNAPSHOT_TIMES, LAYERS, MERIDIAN_POINTS, LONGITUDE_SLOTS), jnp.float32)
    steady_factor = jax.random.uniform(generator_keys[8], (1, LAYERS, MERIDIAN_POINTS, 1), jnp.float32, -1.0, 1.0)
    fluctuating_factor = jax.random.uniform(generator_keys[9], (1, LAYERS, MERIDIAN_POINTS, 1), jnp.float32, 0.2, 1.0)
    poleward_flow = 0.5 * along_latitude_flow + 0.3 * residual_transport_term + 0.7 * steady_share + speed_residual
    potential_warmth = along_latitude_warmth + 0.3 * thermal_deviate + steady_factor * steady_share + 0.5 * steady_warmth + fluctuating_factor * speed_residual + 0.6 * thermal_residual
    return (jnp.clip(poleward_flow, -16.0, 16.0), jnp.clip(potential_warmth, -16.0, 16.0))


def draw_poleward_flow(key, part):
    return ocean_fields(key)[0]


def draw_potential_warmth(key, part):
    return ocean_fields(key)[1]


def draw_water_profile_flag(key, part):
    columns = jnp.arange(LONGITUDE_SLOTS, dtype=jnp.int32)
    threshold = 25 + 65 * columns // LONGITUDE_SLOTS
    dice = jax.random.randint(jax.random.fold_in(key, 21), (MERIDIAN_POINTS, LONGITUDE_SLOTS), 0, 100)
    return (dice < threshold[None, :]).astype(jnp.int32)


def draw_floor_count(key, part):
    wet_levels = jax.random.randint(jax.random.fold_in(key, 31), (MERIDIAN_POINTS, LONGITUDE_SLOTS), 1, LAYERS + 1)
    land_rows = jax.random.randint(jax.random.fold_in(key, 32), (MERIDIAN_POINTS, 1), 0, 16) == 0
    return jnp.where(land_rows, 0, wet_levels).astype(jnp.int32)


def touch_ends(entries, own_key, low, top_value):
    dims = entries.shape
    index_at = [jax.random.randint(jax.random.fold_in(own_key, axis), (), 0, dims[axis]) for axis in range(len(dims))]
    entries = entries.at[tuple(index_at)].set(low)
    longest = dims.index(max(dims))
    index_at[longest] = (index_at[longest] + 1) % dims[longest]
    return entries.at[tuple(index_at)].set(top_value)


def setup_inputs(seed: int = 0) -> dict:
    key_of = jax.random.split(jax.random.key(seed), 6)
    return {
        "poleward_flow": draw_poleward_flow(jax.random.fold_in(key_of[5], 71), 0),
        "potential_warmth": draw_potential_warmth(jax.random.fold_in(key_of[5], 71), 0),
        "water_profile_flag": draw_water_profile_flag(jax.random.fold_in(key_of[5], 71), 0),
        "floor_count": draw_floor_count(jax.random.fold_in(key_of[5], 71), 0),
        "catchment_label_for_site": touch_ends(jax.random.randint(key_of[4], (MERIDIAN_POINTS, LONGITUDE_SLOTS), 0, BASINS), jax.random.fold_in(key_of[4], 1), 0, BASINS - 1).astype(jnp.int32),
    }


highest_accuracy = lax.Precision.HIGHEST

def layer_summands(layer_position, meridional_speed_layer, thermal_layer_slice, bottom_layer_limit, catchment_label_for_site):
    topmost_warmth = jnp.concatenate([thermal_layer_slice[:, 1:, :], jnp.zeros_like(thermal_layer_slice[:, :1, :])], axis=1)
    warmth_entry = 0.5 * (thermal_layer_slice + topmost_warmth)
    upper_depth = jnp.concatenate([bottom_layer_limit[1:], jnp.zeros_like(bottom_layer_limit[:1])], axis=0)
    level_value = layer_position.astype(jnp.float32)
    wet_cells = ((level_value < bottom_layer_limit) & (level_value < upper_depth)).astype(jnp.float32)
    basin_ids = jnp.arange(BASINS, dtype=jnp.int32)
    one_hot = (catchment_label_for_site[None] == basin_ids[:, None, None]).astype(jnp.float32)
    scaling_factors = one_hot * wet_cells[None]
    watered_total = lax.optimization_barrier(jnp.sum(scaling_factors, axis=2))
    along_latitude_flow = jnp.einsum('qfd,zfd->zqf', scaling_factors, meridional_speed_layer, precision=highest_accuracy)
    along_latitude_warmth = jnp.einsum('qfd,zfd->zqf', scaling_factors, warmth_entry, precision=highest_accuracy)
    means_v = along_latitude_flow / jnp.maximum(watered_total, 1.0)
    averages_heat = along_latitude_warmth / jnp.maximum(watered_total, 1.0)
    bar_v = lax.optimization_barrier(jnp.mean(means_v, axis=0))
    bar_t = lax.optimization_barrier(jnp.mean(averages_heat, axis=0))
    mean_velocity = lax.optimization_barrier(jnp.mean(meridional_speed_layer, axis=0))
    average_warmth = lax.optimization_barrier(jnp.mean(warmth_entry, axis=0))
    bar_v_cells = jnp.einsum('bji,bj->ji', one_hot, bar_v, precision=highest_accuracy)
    averaged_heat_grid = jnp.einsum('bji,bj->ji', one_hot, bar_t, precision=highest_accuracy)
    means_v_cells = jnp.einsum('bji,tbj->tji', one_hot, means_v, precision=highest_accuracy)
    averages_heat_grid = jnp.einsum('bji,tbj->tji', one_hot, averages_heat, precision=highest_accuracy)
    velocity_star = mean_velocity - bar_v_cells
    temp_star = average_warmth - averaged_heat_grid
    velocity_eddy = meridional_speed_layer - mean_velocity - (means_v_cells - bar_v_cells)
    warmth_fluctuation = warmth_entry - average_warmth - (averages_heat_grid - averaged_heat_grid)
    scaling = 1.0 / math.sqrt(LONGITUDE_SLOTS)
    mean_flow = scaling * watered_total * bar_v * bar_t
    steady_share = scaling * jnp.einsum('bji,ji->bj', scaling_factors, velocity_star * temp_star, precision=highest_accuracy)
    zonal_swing = scaling * watered_total * lax.optimization_barrier(jnp.mean((means_v - bar_v) * (averages_heat - bar_t), axis=0))
    transient = scaling * jnp.einsum('bji,ji->bj', scaling_factors, lax.optimization_barrier(jnp.mean(velocity_eddy * warmth_fluctuation, axis=0)), precision=highest_accuracy)
    return (wet_cells * temp_star, jnp.stack([mean_flow, steady_share, zonal_swing, transient]))

def reference(poleward_flow, potential_warmth, water_profile_flag, floor_count, catchment_label_for_site):
    bottom_layer_limit = (water_profile_flag * floor_count).astype(jnp.float32)

    def per_level(layer_position):
        meridional_speed_layer = lax.dynamic_index_in_dim(poleward_flow, layer_position, 1, keepdims=False)
        thermal_layer_slice = lax.dynamic_index_in_dim(potential_warmth, layer_position, 1, keepdims=False)
        return layer_summands(layer_position, meridional_speed_layer, thermal_layer_slice, bottom_layer_limit, catchment_label_for_site)
    eddy_temp, stacked = lax.map(per_level, jnp.arange(LAYERS, dtype=jnp.int32))
    return (eddy_temp, jnp.transpose(stacked, (1, 2, 0, 3)))
```

```python
import functools
import math

import jax
import jax.numpy as jnp
from jax import lax
from jax.experimental import pallas as pl
from jax.experimental.pallas import tpu as pltpu
from jax.sharding import PartitionSpec as P

BASINS = 10
GROUP = 16
SUB = 8
LANES = 128
MESH = pl.DeviceIdType.MESH


def kernel(
    dims,
    flow_hbm,
    warmth_hbm,
    flag_hbm,
    floor_hbm,
    label_hbm,
    eddy_ref,
    transport_ref,
    flow,
    warmth,
    flag,
    floor,
    label,
    depth,
    limit,
    mean_warmth,
    split,
    edge,
    edge_in,
    tiles,
    tiles_in,
    bar,
    bar_in,
    flow_sem,
    warmth_sem,
    small_sem,
    edge_send,
    edge_recv,
    tile_send,
    tile_recv,
    bar_send,
    bar_recv,
):
    times, levels, rows, pitch, lats, lons, scaling = dims
    steps = rows // SUB
    lat, lon = lax.axis_index("lat"), lax.axis_index("lon")
    fields = times * levels
    flat_warmth = warmth.reshape(fields * pitch, LANES)

    def flow_copy(n):
        part = pl.ds(pl.multiple_of(n * SUB, SUB), SUB)
        return pltpu.make_async_copy(flow_hbm.at[:, part], flow.at[:, part], flow_sem.at[n])

    def warmth_copy(n):
        part = pl.ds(pl.multiple_of(n * SUB, SUB), SUB)
        return pltpu.make_async_copy(warmth_hbm.at[:, part], warmth.at[:, part], warmth_sem.at[n])

    smalls = [
        pltpu.make_async_copy(flag_hbm, flag, small_sem.at[0]),
        pltpu.make_async_copy(floor_hbm, floor, small_sem.at[1]),
        pltpu.make_async_copy(label_hbm, label, small_sem.at[2]),
    ]
    warmth_copy(0).start()
    for copy in smalls:
        copy.start()
    for n in range(steps):
        if n:
            warmth_copy(n).start()
        flow_copy(n).start()

    barrier = pltpu.get_barrier_semaphore()

    def greet(i, _):
        peer = lax.rem(lon + i, lons)
        pl.semaphore_signal(barrier, inc=1, device_id=(lat, peer), device_id_type=MESH)
        return 0

    lax.fori_loop(1, lons, greet, 0)

    @pl.when(lat < lats - 1)
    def _():
        pl.semaphore_signal(barrier, inc=1, device_id=(lat + 1, lon), device_id_type=MESH)

    for copy in smalls:
        copy.wait()
    warmth_copy(0).wait()
    depth[0:rows, :] = flag[...] * floor[...]
    for a in range(fields // SUB):
        edge[a * SUB : (a + 1) * SUB, :] = flat_warmth[pl.ds(a * SUB * pitch, SUB, stride=pitch), :]
    edge[fields : fields + SUB, :] = depth[0:SUB, :].astype(jnp.float32)
    tiles_in[pl.ds(pl.multiple_of(lon * SUB, SUB), SUB), :] = jnp.zeros((SUB, LANES), jnp.float32)

    edge_copy = pltpu.make_async_remote_copy(
        src_ref=edge,
        dst_ref=edge_in,
        send_sem=edge_send,
        recv_sem=edge_recv,
        device_id=(lat - 1, lon),
        device_id_type=MESH,
    )
    pl.semaphore_wait(barrier, jnp.where(lat > 0, lons, lons - 1))

    @pl.when(lat > 0)
    def _():
        edge_copy.start()

    lane = lax.broadcasted_iota(jnp.int32, (SUB, LANES), 1)
    sub = lax.broadcasted_iota(jnp.int32, (SUB, LANES), 0)

    def step(n):
        row = pl.multiple_of(n * SUB, SUB)
        here = pl.ds(row, SUB)
        next_depth = depth[pl.ds(row + 1, SUB), :]
        lim = jnp.minimum(depth[here, :], next_depth)
        limit[here, :] = lim
        for k in range(levels):
            wet = jnp.where(lim > k, 1.0, 0.0)
            v = [flow[t * levels + k, here, :] for t in range(times)]
            w = [
                0.5
                * (
                    warmth[t * levels + k, here, :]
                    + flat_warmth[pl.ds((t * levels + k) * pitch + row + 1, SUB), :]
                )
                for t in range(times)
            ]
            mean_v = functools.reduce(jnp.add, v) * (1.0 / times)
            mean_w = functools.reduce(jnp.add, w) * (1.0 / times)
            mean_warmth[k, here, :] = mean_w
            cross = functools.reduce(
                jnp.add, [(v[t] - mean_v) * (w[t] - mean_w) for t in range(times)]
            ) * (1.0 / times)
            chunks = [x * wet for x in v] + [x * wet for x in w]
            chunks += [wet, mean_v * mean_w * wet, cross * wet, jnp.zeros_like(wet)]
            for c in range(0, len(chunks), 2):
                both = jnp.concatenate(chunks[c : c + 2], axis=0)
                high = both.astype(jnp.bfloat16)
                low = (both - high.astype(jnp.float32)).astype(jnp.bfloat16)
                at = (k * len(chunks) + c) * SUB
                split[at : at + 2 * SUB, 0:LANES] = high
                split[at : at + 2 * SUB, LANES : 2 * LANES] = low
        iota = lax.broadcasted_iota(jnp.int32, (GROUP, LANES), 0)
        tags = label[here, :]
        hot = jnp.concatenate(
            [
                jnp.where(
                    jnp.broadcast_to(tags[r : r + 1, :], (GROUP, LANES)) == iota,
                    1.0,
                    0.0,
                )
                for r in (0, *range(SUB - 1, 0, -1))
            ],
            axis=0,
        ).astype(jnp.bfloat16)
        hot = jnp.concatenate([hot, hot], axis=1)
        out = lax.dot_general(
            split[...], hot, (((1,), (1,)), ((), ())), preferred_element_type=jnp.float32
        )
        width = 2 * times + 4
        slots = times + 2

        def piece(k, c, m):
            x = out[(k * width + c) * SUB : (k * width + c + 1) * SUB, :]
            return pltpu.roll(x, 10 * m, axis=1) if m else x

        turned = (lane + GROUP * sub) % LANES
        marks = [(turned >= 10 * m) & (turned < 10 * m + 10) for m in range(slots)]
        for k in range(levels):
            count = piece(k, 2 * times, times)
            for half in range(2):
                acc = jnp.where(marks[times], count, 0.0)
                for t in range(times):
                    acc = jnp.where(marks[t], piece(k, half * times + t, t), acc)
                acc = jnp.where(marks[times + 1], piece(k, 2 * times + 1 + half, times + 1), acc)
                tiles[pl.ds(row * SUB + half * levels + k, SUB, stride=SUB), :] = pltpu.roll(
                    acc, 0, axis=1, stride=GROUP, stride_axis=0
                )

    def early(n, _):
        warmth_copy(n + 1).wait()
        flow_copy(n).wait()
        step(n)
        return 0

    lax.fori_loop(0, steps - 1, early, 0)
    flow_copy(steps - 1).wait()

    @pl.when(lat < lats - 1)
    def _():
        edge_copy.wait_recv()
        for a in range(fields // SUB):
            flat_warmth[pl.ds(a * SUB * pitch + rows, SUB, stride=pitch), :] = edge_in[
                a * SUB : (a + 1) * SUB, :
            ]
        depth[rows : rows + SUB, :] = edge_in[fields : fields + SUB, :].astype(jnp.int32)

    @pl.when(lat == lats - 1)
    def _():
        for a in range(fields // SUB):
            flat_warmth[pl.ds(a * SUB * pitch + rows, SUB, stride=pitch), :] = jnp.zeros(
                (SUB, LANES), jnp.float32
            )
        depth[rows : rows + SUB, :] = jnp.zeros((SUB, LANES), jnp.int32)

    step(steps - 1)

    mine = pl.ds(pl.multiple_of(lon * SUB, SUB), SUB)

    def send_tile(i, _):
        peer = lax.rem(lon + i, lons)
        pltpu.make_async_remote_copy(
            src_ref=tiles.at[pl.ds(pl.multiple_of(peer * SUB, SUB), SUB)],
            dst_ref=tiles_in.at[mine],
            send_sem=tile_send,
            recv_sem=tile_recv,
            device_id=(lat, peer),
            device_id_type=MESH,
        ).start()
        return 0

    lax.fori_loop(1, lons, send_tile, 0)
    others = pl.ds(0, (lons - 1) * SUB)
    all_tiles = pltpu.make_async_remote_copy(
        src_ref=tiles.at[others],
        dst_ref=tiles_in.at[others],
        send_sem=tile_send,
        recv_sem=tile_recv,
        device_id=(lat, lon),
        device_id_type=MESH,
    )
    all_tiles.wait_recv()
    parts = [tiles[mine, :]] + [tiles_in[SUB * p : SUB * p + SUB, :] for p in range(lons)]
    while len(parts) > 1:
        parts = [sum(parts[i : i + 2][1:], parts[i]) for i in range(0, len(parts), 2)]
    total = parts[0]

    def moved(x, lanes):
        return pltpu.roll(x, (-lanes) % LANES, axis=1)

    count = moved(total, 10 * times)
    first = lane < BASINS
    divisor = jnp.maximum(count, 1.0)
    sums = total
    for t in range(1, times):
        sums = sums + moved(total, 10 * t)
    bars = jnp.where(first, sums / divisor * (1.0 / times), 0.0)
    spread = pltpu.roll(bars, 0, axis=1, stride=10, stride_axis=0)
    for shift in (4, 2, 1):
        spread = spread + pltpu.roll(spread, shift, axis=0)
    bar[...] = spread[0:1, :]
    bar_in[pl.ds(lon, 1)] = spread[0:1, :].reshape(1, 1, LANES)

    def send_bar(i, _):
        peer = lax.rem(lon + i, lons)
        pltpu.make_async_remote_copy(
            src_ref=bar,
            dst_ref=bar_in.at[lon],
            send_sem=bar_send,
            recv_sem=bar_recv,
            device_id=(lat, peer),
            device_id_type=MESH,
        ).start()
        return 0

    lax.fori_loop(1, lons, send_bar, 0)

    def other_half(x):
        return pltpu.roll(x, levels, axis=0)

    bars_w = other_half(bars)
    flow_part = scaling * count * bars * bars_w
    swing = jnp.zeros_like(total)
    for t in range(times):
        dev = (moved(total, 10 * t) if t else total) / divisor - bars
        swing = swing + dev * other_half(dev)
    swing = scaling * count * (swing * (1.0 / times))
    both = moved(total, 10 * (times + 1))
    steady = scaling * both - flow_part
    transient = scaling * other_half(both) - swing
    for q, value in enumerate((flow_part, steady, swing, transient)):
        for k in range(levels):
            transport_ref[q, k] = value[k : k + 1, 0:BASINS]

    every_bar = pltpu.make_async_remote_copy(
        src_ref=bar_in.at[pl.ds(0, lons - 1)],
        dst_ref=bar_in.at[pl.ds(0, lons - 1)],
        send_sem=bar_send,
        recv_sem=bar_recv,
        device_id=(lat, lon),
        device_id_type=MESH,
    )
    every_bar.wait_recv()
    for n in range(steps):
        here = slice(n * SUB, (n + 1) * SUB)
        table = bar_in[here].reshape(SUB, LANES)
        lim = limit[here, :]
        tags = label[here, :]
        for k in range(levels):
            cell = jnp.take_along_axis(
                table, tags + (levels * 10 + k * 10), axis=1, mode="promise_in_bounds"
            )
            eddy_ref[k, here, :] = jnp.where(lim > k, mean_warmth[k, here, :] - cell, 0.0)

    all_tiles.wait_send()
    every_bar.wait_send()

    @pl.when(lat > 0)
    def _():
        edge_copy.wait_send()


def shards(lats, lons, flow, warmth, flag, floor, label):
    times, levels, rows, cols = flow.shape
    fields = times * levels
    pitch = rows + SUB
    scaling = 1.0 / math.sqrt(cols * lons)
    dims = (times, levels, rows, pitch, lats, lons, scaling)
    anywhere = pl.BlockSpec(memory_space=pl.ANY)
    local = pl.BlockSpec(memory_space=pltpu.VMEM)
    dma = pltpu.SemaphoreType.DMA
    f32 = jnp.float32
    eddy, transport = pl.pallas_call(
        functools.partial(kernel, dims),
        out_shape=(
            jax.ShapeDtypeStruct((levels, rows, cols), f32),
            jax.ShapeDtypeStruct((4, levels, 1, BASINS), f32),
        ),
        in_specs=[anywhere] * 5,
        out_specs=(local, local),
        scratch_shapes=[
            pltpu.VMEM((fields, rows, cols), f32),
            pltpu.VMEM((fields, pitch, cols), f32),
            pltpu.VMEM((rows, cols), jnp.int32),
            pltpu.VMEM((rows, cols), jnp.int32),
            pltpu.VMEM((rows, cols), jnp.int32),
            pltpu.VMEM((pitch, cols), jnp.int32),
            pltpu.VMEM((rows, cols), jnp.int32),
            pltpu.VMEM((levels, rows, cols), f32),
            pltpu.VMEM((levels * (2 * times + 4) * SUB, 2 * cols), jnp.bfloat16),
            pltpu.VMEM((fields + SUB, cols), f32),
            pltpu.VMEM((fields + SUB, cols), f32),
            pltpu.VMEM((rows * SUB, cols), f32),
            pltpu.VMEM((rows * SUB, cols), f32),
            pltpu.VMEM((1, cols), f32),
            pltpu.VMEM((rows, 1, cols), f32),
            dma((rows // SUB,)),
            dma((rows // SUB,)),
            dma((3,)),
            dma,
            dma,
            dma,
            dma,
            dma,
            dma,
        ],
        compiler_params=pltpu.CompilerParams(collective_id=0, has_side_effects=True),
    )(
        flow.reshape(fields, rows, cols),
        warmth.reshape(fields, rows, cols),
        flag,
        floor,
        label,
    )
    return eddy, jnp.transpose(transport, (0, 3, 1, 2))


def solution(mesh):
    return jax.shard_map(
        functools.partial(shards, mesh.shape["lat"], mesh.shape["lon"]),
        mesh=mesh,
        in_specs=(
            P(None, None, "lat", "lon"),
            P(None, None, "lat", "lon"),
            P("lat", "lon"),
            P("lat", "lon"),
            P("lat", "lon"),
        ),
        out_specs=(P(None, "lat", "lon"), P(None, None, None, ("lat", "lon"))),
        check_vma=False,
    )
```

```python
import functools
import itertools
import math

import jax
import jax.numpy as jnp
from jax import lax
from jax.experimental import pallas as pl
from jax.experimental.pallas import tpu as pltpu
from jax.sharding import PartitionSpec as P

BASINS = 10
FAN = 4
GROUP = 16
SUB = 8
LANES = 128
MESH = pl.DeviceIdType.MESH


def kernel(
    dims,
    flow_hbm,
    warmth_hbm,
    flag_hbm,
    floor_hbm,
    label_hbm,
    eddy_ref,
    transport_ref,
    flow,
    warmth,
    flag,
    floor,
    label,
    depth,
    limit,
    mean_warmth,
    split_even,
    split_odd,
    edge,
    edge_in,
    tiles,
    tiles_in,
    bar,
    bar_in,
    flow_sem,
    warmth_sem,
    small_sem,
    edge_send,
    edge_recv,
    tile_send,
    tile_recv,
    bar_send,
    bar_recv,
    met_sem,
):
    splits = (split_even, split_odd)
    times, levels, rows, pitch, lats, lons, scaling = dims
    steps = rows // SUB
    lat, lon = lax.axis_index("lat"), lax.axis_index("lon")
    fields = times * levels
    places = round(math.log(lons, FAN))
    flat_warmth = warmth.reshape(fields * pitch, LANES)

    def flow_copy(n):
        part = pl.ds(pl.multiple_of(n * SUB, SUB), SUB)
        return pltpu.make_async_copy(flow_hbm.at[:, part], flow.at[:, part], flow_sem.at[n])

    def warmth_copy(n):
        part = pl.ds(pl.multiple_of(n * SUB, SUB), SUB)
        return pltpu.make_async_copy(warmth_hbm.at[:, part], warmth.at[:, part], warmth_sem.at[n])

    smalls = [
        pltpu.make_async_copy(flag_hbm, flag, small_sem.at[0]),
        pltpu.make_async_copy(floor_hbm, floor, small_sem.at[1]),
        pltpu.make_async_copy(label_hbm, label, small_sem.at[2]),
    ]
    warmth_copy(0).start()
    for copy in smalls:
        copy.start()
    for n in range(steps):
        if n:
            warmth_copy(n).start()
        flow_copy(n).start()

    barrier = pltpu.get_barrier_semaphore()
    digits = [lon // FAN**d % FAN for d in range(places)]
    turned_digits = [
        [lax.rem(digits[d] + i, FAN) * FAN**d for i in range(FAN)] for d in range(places)
    ]

    def signal_line(semaphore, d):
        rest = lon - turned_digits[d][0]
        for i in range(1, FAN):
            pl.semaphore_signal(
                semaphore,
                inc=1,
                device_id=(lat, rest + turned_digits[d][i]),
                device_id_type=MESH,
            )

    for d in range(places):
        signal_line(barrier, d)

    @pl.when(lat < lats - 1)
    def _():
        pl.semaphore_signal(barrier, inc=1, device_id=(lat + 1, lon), device_id_type=MESH)

    for copy in smalls:
        copy.wait()
    warmth_copy(0).wait()
    depth[0:rows, :] = flag[...] * floor[...]
    for a in range(fields // SUB):
        edge[a * SUB : (a + 1) * SUB, :] = flat_warmth[pl.ds(a * SUB * pitch, SUB, stride=pitch), :]
    edge[fields : fields + SUB, :] = depth[0:SUB, :].astype(jnp.float32)
    tiles_in[pl.ds(pl.multiple_of(lon * SUB, SUB), SUB), :] = jnp.zeros((SUB, LANES), jnp.float32)

    edge_copy = pltpu.make_async_remote_copy(
        src_ref=edge,
        dst_ref=edge_in,
        send_sem=edge_send,
        recv_sem=edge_recv,
        device_id=(lat - 1, lon),
        device_id_type=MESH,
    )
    met = places * (FAN - 1)
    pl.semaphore_wait(barrier, jnp.where(lat > 0, met + 1, met))

    @pl.when(lat > 0)
    def _():
        edge_copy.start()

    signal_line(met_sem.at[1], 1)

    lane = lax.broadcasted_iota(jnp.int32, (SUB, LANES), 1)
    sub = lax.broadcasted_iota(jnp.int32, (SUB, LANES), 0)

    def prepare(n):
        row = n * SUB
        here = pl.ds(row, SUB)
        split = splits[n % 2]
        next_depth = depth[pl.ds(row + 1, SUB), :]
        lim = jnp.minimum(depth[here, :], next_depth)
        limit[here, :] = lim
        for k in range(levels):
            wet = jnp.where(lim > k, 1.0, 0.0)
            v = [flow[t * levels + k, here, :] for t in range(times)]
            w = [
                0.5
                * (
                    warmth[t * levels + k, here, :]
                    + flat_warmth[pl.ds((t * levels + k) * pitch + row + 1, SUB), :]
                )
                for t in range(times)
            ]
            mean_v = functools.reduce(jnp.add, v) * (1.0 / times)
            mean_w = functools.reduce(jnp.add, w) * (1.0 / times)
            mean_warmth[k, here, :] = mean_w
            cross = functools.reduce(
                jnp.add, [(v[t] - mean_v) * (w[t] - mean_w) for t in range(times)]
            ) * (1.0 / times)
            chunks = [x * wet for x in v] + [x * wet for x in w]
            chunks += [wet, mean_v * mean_w * wet, cross * wet, jnp.zeros_like(wet)]
            for c in range(0, len(chunks), 2):
                both = jnp.concatenate(chunks[c : c + 2], axis=0)
                high = both.astype(jnp.bfloat16)
                low = (both - high.astype(jnp.float32)).astype(jnp.bfloat16)
                at = (k * len(chunks) + c) * SUB
                split[at : at + 2 * SUB, 0:LANES] = high
                split[at : at + 2 * SUB, LANES : 2 * LANES] = low
    def contract(n):
        row = n * SUB
        here = pl.ds(row, SUB)
        split = splits[n % 2]
        iota = lax.broadcasted_iota(jnp.int32, (GROUP, LANES), 0)
        tags = label[here, :]
        hot = jnp.concatenate(
            [
                jnp.where(
                    jnp.broadcast_to(tags[r : r + 1, :], (GROUP, LANES)) == iota,
                    1.0,
                    0.0,
                )
                for r in (0, *range(SUB - 1, 0, -1))
            ],
            axis=0,
        ).astype(jnp.bfloat16)
        hot = jnp.concatenate([hot, hot], axis=1)
        out = lax.dot_general(
            split[...], hot, (((1,), (1,)), ((), ())), preferred_element_type=jnp.float32
        )
        width = 2 * times + 4
        slots = times + 2

        def piece(k, c, m):
            x = out[(k * width + c) * SUB : (k * width + c + 1) * SUB, :]
            return pltpu.roll(x, 10 * m, axis=1) if m else x

        turned = (lane + GROUP * sub) % LANES
        marks = [(turned >= 10 * m) & (turned < 10 * m + 10) for m in range(slots)]
        for k in range(levels):
            count = piece(k, 2 * times, times)
            for half in range(2):
                acc = jnp.where(marks[times], count, 0.0)
                for t in range(times):
                    acc = jnp.where(marks[t], piece(k, half * times + t, t), acc)
                acc = jnp.where(marks[times + 1], piece(k, 2 * times + 1 + half, times + 1), acc)
                tiles[pl.ds(row * SUB + half * levels + k, SUB, stride=SUB), :] = pltpu.roll(
                    acc, 0, axis=1, stride=GROUP, stride_axis=0
                )

    for n in range(steps - 1):
        warmth_copy(n + 1).wait()
        flow_copy(n).wait()
        prepare(n)
        if n:
            contract(n - 1)
        for d in range(2, places):
            if n == 2 * d:
                pl.semaphore_wait(met_sem.at[d - 1], FAN - 1)
                signal_line(met_sem.at[d], d)
    flow_copy(steps - 1).wait()

    @pl.when(lat < lats - 1)
    def _():
        edge_copy.wait_recv()
        for a in range(fields // SUB):
            flat_warmth[pl.ds(a * SUB * pitch + rows, SUB, stride=pitch), :] = edge_in[
                a * SUB : (a + 1) * SUB, :
            ]
        depth[rows : rows + SUB, :] = edge_in[fields : fields + SUB, :].astype(jnp.int32)

    @pl.when(lat == lats - 1)
    def _():
        for a in range(fields // SUB):
            flat_warmth[pl.ds(a * SUB * pitch + rows, SUB, stride=pitch), :] = jnp.zeros(
                (SUB, LANES), jnp.float32
            )
        depth[rows : rows + SUB, :] = jnp.zeros((SUB, LANES), jnp.int32)

    prepare(steps - 1)
    contract(steps - 2)
    contract(steps - 1)
    pl.semaphore_wait(met_sem.at[places - 1], FAN - 1)

    mine = pl.ds(pl.multiple_of(lon * SUB, SUB), SUB)

    def far_first():
        ways = itertools.product(range(FAN), repeat=places)
        hops = lambda way: sum(min(i, FAN - i) for i in way[1:]) + (way[0] > 0)
        for way in sorted(ways, key=hops, reverse=True):
            if any(way):
                yield sum(turned_digits[d][way[d]] for d in range(places))

    for peer in far_first():
        pltpu.make_async_remote_copy(
            src_ref=tiles.at[pl.ds(pl.multiple_of(peer * SUB, SUB), SUB)],
            dst_ref=tiles_in.at[mine],
            send_sem=tile_send,
            recv_sem=tile_recv,
            device_id=(lat, peer),
            device_id_type=MESH,
        ).start()
    others = pl.ds(0, (lons - 1) * SUB)
    all_tiles = pltpu.make_async_remote_copy(
        src_ref=tiles.at[others],
        dst_ref=tiles_in.at[others],
        send_sem=tile_send,
        recv_sem=tile_recv,
        device_id=(lat, lon),
        device_id_type=MESH,
    )
    all_tiles.wait_recv()
    parts = [tiles[mine, :]] + [tiles_in[SUB * p : SUB * p + SUB, :] for p in range(lons)]
    while len(parts) > 1:
        parts = [sum(parts[i : i + 2][1:], parts[i]) for i in range(0, len(parts), 2)]
    total = parts[0]

    def moved(x, lanes):
        return pltpu.roll(x, (-lanes) % LANES, axis=1)

    count = moved(total, 10 * times)
    first = lane < BASINS
    divisor = jnp.maximum(count, 1.0)
    sums = total
    for t in range(1, times):
        sums = sums + moved(total, 10 * t)
    bars = jnp.where(first, sums / divisor * (1.0 / times), 0.0)
    spread = pltpu.roll(bars, 0, axis=1, stride=10, stride_axis=0)
    for shift in (4, 2, 1):
        spread = spread + pltpu.roll(spread, shift, axis=0)
    bar[...] = spread[0:1, :]
    bar_in[pl.ds(lon, 1)] = spread[0:1, :].reshape(1, 1, LANES)

    for peer in far_first():
        pltpu.make_async_remote_copy(
            src_ref=bar,
            dst_ref=bar_in.at[lon],
            send_sem=bar_send,
            recv_sem=bar_recv,
            device_id=(lat, peer),
            device_id_type=MESH,
        ).start()

    def other_half(x):
        return pltpu.roll(x, levels, axis=0)

    bars_w = other_half(bars)
    flow_part = scaling * count * bars * bars_w
    swing = jnp.zeros_like(total)
    for t in range(times):
        dev = (moved(total, 10 * t) if t else total) / divisor - bars
        swing = swing + dev * other_half(dev)
    swing = scaling * count * (swing * (1.0 / times))
    both = moved(total, 10 * (times + 1))
    steady = scaling * both - flow_part
    transient = scaling * other_half(both) - swing
    for q, value in enumerate((flow_part, steady, swing, transient)):
        for k in range(levels):
            transport_ref[q, k] = value[k : k + 1, 0:BASINS]

    every_bar = pltpu.make_async_remote_copy(
        src_ref=bar_in.at[pl.ds(0, lons - 1)],
        dst_ref=bar_in.at[pl.ds(0, lons - 1)],
        send_sem=bar_send,
        recv_sem=bar_recv,
        device_id=(lat, lon),
        device_id_type=MESH,
    )
    every_bar.wait_recv()
    for n in range(steps):
        here = slice(n * SUB, (n + 1) * SUB)
        table = bar_in[here].reshape(SUB, LANES)
        lim = limit[here, :]
        tags = label[here, :]
        for k in range(levels):
            cell = jnp.take_along_axis(
                table, tags + (levels * 10 + k * 10), axis=1, mode="promise_in_bounds"
            )
            eddy_ref[k, here, :] = jnp.where(lim > k, mean_warmth[k, here, :] - cell, 0.0)

    all_tiles.wait_send()
    every_bar.wait_send()

    @pl.when(lat > 0)
    def _():
        edge_copy.wait_send()


def write_out(eddy, transport, eddy_out, transport_out, sem):
    copies = [
        pltpu.make_async_copy(eddy, eddy_out, sem.at[0]),
        pltpu.make_async_copy(transport, transport_out, sem.at[1]),
    ]
    for copy in copies:
        copy.start()
    for copy in copies:
        copy.wait()


def shards(lats, lons, flow, warmth, flag, floor, label):
    times, levels, rows, cols = flow.shape
    fields = times * levels
    pitch = rows + SUB
    scaling = 1.0 / math.sqrt(cols * lons)
    dims = (times, levels, rows, pitch, lats, lons, scaling)
    local = pl.BlockSpec(memory_space=pltpu.VMEM)
    dma = pltpu.SemaphoreType.DMA
    f32 = jnp.float32
    eddy, transport = pl.pallas_call(
        functools.partial(kernel, dims),
        out_shape=(
            pltpu.VMEM((levels, rows, cols), f32),
            pltpu.VMEM((4, levels, 1, BASINS), f32),
        ),
        in_specs=[pl.BlockSpec(memory_space=pltpu.HBM)] * 5,
        out_specs=(local, local),
        scratch_shapes=[
            pltpu.VMEM((fields, rows, cols), f32),
            pltpu.VMEM((fields, pitch, cols), f32),
            pltpu.VMEM((rows, cols), jnp.int32),
            pltpu.VMEM((rows, cols), jnp.int32),
            pltpu.VMEM((rows, cols), jnp.int32),
            pltpu.VMEM((pitch, cols), jnp.int32),
            pltpu.VMEM((rows, cols), jnp.int32),
            pltpu.VMEM((levels, rows, cols), f32),
            pltpu.VMEM((levels * (2 * times + 4) * SUB, 2 * cols), jnp.bfloat16),
            pltpu.VMEM((levels * (2 * times + 4) * SUB, 2 * cols), jnp.bfloat16),
            pltpu.VMEM((fields + SUB, cols), f32),
            pltpu.VMEM((fields + SUB, cols), f32),
            pltpu.VMEM((rows * SUB, cols), f32),
            pltpu.VMEM((rows * SUB, cols), f32),
            pltpu.VMEM((1, cols), f32),
            pltpu.VMEM((rows, 1, cols), f32),
            dma((rows // SUB,)),
            dma((rows // SUB,)),
            dma((3,)),
            dma,
            dma,
            dma,
            dma,
            dma,
            dma,
            pltpu.SemaphoreType.REGULAR((round(math.log(lons, FAN)),)),
        ],
        compiler_params=pltpu.CompilerParams(
            collective_id=0, has_side_effects=True, vmem_limit_bytes=66879488
        ),
    )(
        flow.reshape(fields, rows, cols),
        warmth.reshape(fields, rows, cols),
        flag,
        floor,
        label,
    )
    eddy, transport = pl.pallas_call(
        write_out,
        out_shape=tuple(jax.ShapeDtypeStruct(a.shape, a.dtype) for a in (eddy, transport)),
        in_specs=[local] * 2,
        out_specs=[pl.BlockSpec(memory_space=pltpu.HBM)] * 2,
        scratch_shapes=[dma((2,))],
        compiler_params=pltpu.CompilerParams(vmem_limit_bytes=2**20),
    )(eddy, transport)
    return eddy, jnp.transpose(transport, (0, 3, 1, 2))


def solution(mesh):
    return jax.shard_map(
        functools.partial(shards, mesh.shape["lat"], mesh.shape["lon"]),
        mesh=mesh,
        in_specs=(
            P(None, None, "lat", "lon"),
            P(None, None, "lat", "lon"),
            P("lat", "lon"),
            P("lat", "lon"),
            P("lat", "lon"),
        ),
        out_specs=(P(None, "lat", "lon"), P(None, None, None, ("lat", "lon"))),
        check_vma=False,
    )
```

```python
import functools
import itertools
import math

import jax
import jax.numpy as jnp
from jax import lax
from jax.experimental import pallas as pl
from jax.experimental.pallas import tpu as pltpu
from jax.sharding import PartitionSpec as P

BASINS = 10
FAN = 4
GROUP = 16
SUB = 8
LANES = 128
MESH = pl.DeviceIdType.MESH


def kernel(
    dims,
    flow_hbm,
    warmth_hbm,
    flag_hbm,
    floor_hbm,
    label_hbm,
    eddy_ref,
    transport_ref,
    flow,
    warmth,
    flag,
    floor,
    label,
    depth,
    limit,
    mean_warmth,
    split_even,
    split_odd,
    edge,
    edge_in,
    tiles,
    tiles_in,
    bar,
    bar_in,
    edge_line,
    edge_lines,
    lines,
    lines_in,
    flow_sem,
    warmth_sem,
    small_sem,
    edge_send,
    edge_recv,
    tile_send,
    tile_recv,
    bar_send,
    bar_recv,
    line_send,
    line_recv,
    edge_line_send,
    edge_line_recv,
    met_sem,
):
    splits = (split_even, split_odd)
    times, levels, rows, pitch, lats, lons, scaling = dims
    steps = rows // SUB
    lat, lon = lax.axis_index("lat"), lax.axis_index("lon")
    fields = times * levels
    last = rows - 1
    mine = pl.ds(pl.multiple_of(lon * SUB, SUB), SUB)
    places = round(math.log(lons, FAN))
    flat_flow = flow.reshape(fields * rows, LANES)
    flat_mean = mean_warmth.reshape(levels * rows, LANES)
    flat_warmth = warmth.reshape(fields * pitch, LANES)

    def flow_copy(n):
        part = pl.ds(pl.multiple_of(n * SUB, SUB), SUB)
        return pltpu.make_async_copy(flow_hbm.at[:, part], flow.at[:, part], flow_sem.at[n])

    def warmth_copy(n):
        part = pl.ds(pl.multiple_of(n * SUB, SUB), SUB)
        return pltpu.make_async_copy(warmth_hbm.at[:, part], warmth.at[:, part], warmth_sem.at[n])

    smalls = [
        pltpu.make_async_copy(flag_hbm, flag, small_sem.at[0]),
        pltpu.make_async_copy(floor_hbm, floor, small_sem.at[1]),
        pltpu.make_async_copy(label_hbm, label, small_sem.at[2]),
    ]
    warmth_copy(0).start()
    for copy in smalls:
        copy.start()

    barrier = pltpu.get_barrier_semaphore()
    turned_digits = [
        [lax.rem(lon // FAN**d + i, FAN) * FAN**d for i in range(FAN)] for d in range(places)
    ]

    def far_first():
        ways = itertools.product(range(FAN), repeat=places)
        hops = lambda way: sum(min(i, FAN - i) for i in way[1:]) + (way[0] > 0)
        return [way for way in sorted(ways, key=hops, reverse=True) if any(way)]

    def at(way):
        return sum(turned_digits[d][way[d]] for d in range(places))

    def across(way):
        return way[1] > 0 and not any(way[:1] + way[2:])

    greeted = [way for way in far_first() if across(way) or way[1] == 0]
    for way in greeted:
        pl.semaphore_signal(barrier, inc=1, device_id=(lat, at(way)), device_id_type=MESH)

    @pl.when(lat < lats - 1)
    def _():
        pl.semaphore_signal(barrier, inc=1, device_id=(lat + 1, lon), device_id_type=MESH)

    for n in range(steps):
        if n:
            warmth_copy(n).start()
        flow_copy(n).start()
    for a in range(fields // SUB):
        flat_warmth[pl.ds(a * SUB * pitch + rows, SUB, stride=pitch), :] = jnp.zeros(
            (SUB, LANES), jnp.float32
        )
    depth[rows : rows + SUB, :] = jnp.zeros((SUB, LANES), jnp.int32)
    tiles_in[mine, :] = jnp.zeros((SUB, LANES), jnp.float32)
    for copy in smalls:
        copy.wait()
    warmth_copy(0).wait()
    depth[0:rows, :] = flag[...] * floor[...]
    for a in range(fields // SUB):
        edge[a * SUB : (a + 1) * SUB, :] = flat_warmth[pl.ds(a * SUB * pitch, SUB, stride=pitch), :]
    edge[fields : fields + SUB, :] = depth[0:SUB, :].astype(jnp.float32)

    edge_copy = pltpu.make_async_remote_copy(
        src_ref=edge,
        dst_ref=edge_in,
        send_sem=edge_send,
        recv_sem=edge_recv,
        device_id=(lat - 1, lon),
        device_id_type=MESH,
    )
    met = len(greeted)
    pl.semaphore_wait(barrier, jnp.where(lat > 0, met + 1, met))

    @pl.when(lat > 0)
    def _():
        edge_copy.start()

    for way in greeted:
        if across(way):
            pl.semaphore_signal(met_sem, inc=1, device_id=(lat, at(way)), device_id_type=MESH)

    lane = lax.broadcasted_iota(jnp.int32, (SUB, LANES), 1)
    sub = lax.broadcasted_iota(jnp.int32, (SUB, LANES), 0)

    def prepare(n):
        row = n * SUB
        here = pl.ds(row, SUB)
        split = splits[n % 2]
        next_depth = depth[pl.ds(row + 1, SUB), :]
        lim = jnp.minimum(depth[here, :], next_depth)
        limit[here, :] = lim
        for k in range(levels):
            wet = jnp.where(lim > k, 1.0, 0.0)
            v = [flow[t * levels + k, here, :] for t in range(times)]
            w = [
                0.5
                * (
                    warmth[t * levels + k, here, :]
                    + flat_warmth[pl.ds((t * levels + k) * pitch + row + 1, SUB), :]
                )
                for t in range(times)
            ]
            mean_v = functools.reduce(jnp.add, v) * (1.0 / times)
            mean_w = functools.reduce(jnp.add, w) * (1.0 / times)
            mean_warmth[k, here, :] = mean_w
            cross = functools.reduce(
                jnp.add, [(v[t] - mean_v) * (w[t] - mean_w) for t in range(times)]
            ) * (1.0 / times)
            chunks = [x * wet for x in v] + [x * wet for x in w]
            chunks += [wet, mean_v * mean_w * wet, cross * wet, mean_w * wet]
            for c in range(0, len(chunks), 2):
                both = jnp.concatenate(chunks[c : c + 2], axis=0)
                high = both.astype(jnp.bfloat16)
                low = (both - high.astype(jnp.float32)).astype(jnp.bfloat16)
                at = (k * len(chunks) + c) * SUB
                split[at : at + 2 * SUB, 0:LANES] = high
                split[at : at + 2 * SUB, LANES : 2 * LANES] = low
    def contract(n):
        row = n * SUB
        here = pl.ds(row, SUB)
        split = splits[n % 2]
        iota = lax.broadcasted_iota(jnp.int32, (GROUP, LANES), 0)
        tags = label[here, :]
        hot = jnp.concatenate(
            [
                jnp.where(
                    jnp.broadcast_to(tags[r : r + 1, :], (GROUP, LANES)) == iota,
                    1.0,
                    0.0,
                )
                for r in (0, *range(SUB - 1, 0, -1))
            ],
            axis=0,
        ).astype(jnp.bfloat16)
        hot = jnp.concatenate([hot, hot], axis=1)
        out = lax.dot_general(
            split[...], hot, (((1,), (1,)), ((), ())), preferred_element_type=jnp.float32
        )
        width = 2 * times + 4
        slots = times + 2

        def piece(k, c, m):
            x = out[(k * width + c) * SUB : (k * width + c + 1) * SUB, :]
            return pltpu.roll(x, 10 * m, axis=1) if m else x

        turned = (lane + GROUP * sub) % LANES
        marks = [(turned >= 10 * m) & (turned < 10 * m + 10) for m in range(slots)]
        line = jnp.zeros_like(lane, jnp.float32)
        for k in range(levels):
            line = jnp.where(marks[k], piece(k, 2 * times, k), line)
            line = jnp.where(marks[levels + k], piece(k, width - 1, levels + k), line)
        line = pltpu.roll(line, 0, axis=1, stride=GROUP, stride_axis=0)
        lines[here] = line.reshape(SUB, 1, LANES)
        for k in range(levels):
            count = piece(k, 2 * times, times)
            for half in range(2):
                acc = jnp.where(marks[times], count, 0.0)
                for t in range(times):
                    acc = jnp.where(marks[t], piece(k, half * times + t, t), acc)
                acc = jnp.where(marks[times + 1], piece(k, 2 * times + 1 + half, times + 1), acc)
                tiles[pl.ds(row * SUB + half * levels + k, SUB, stride=SUB), :] = pltpu.roll(
                    acc, 0, axis=1, stride=GROUP, stride_axis=0
                )

    def edge_sums():
        lim = jnp.minimum(
            depth[last : last + 1, :], edge_in[fields : fields + 1, :].astype(jnp.int32)
        )
        limit[last : last + 1, :] = lim
        wet = jnp.where(jnp.broadcast_to(lim, (SUB, LANES)) > sub % levels, 1.0, 0.0)
        x = []
        for t in range(times):
            v = flat_flow[pl.ds(t * levels * rows + last, levels, stride=rows), :]
            w = flat_warmth[pl.ds(t * levels * pitch + last, levels, stride=pitch), :]
            w = 0.5 * (w + edge_in[t * levels : (t + 1) * levels, :])
            x.append(jnp.concatenate([v, w], axis=0))
        mean = functools.reduce(jnp.add, x) * (1.0 / times)
        flat_mean[pl.ds(last, levels, stride=rows), :] = mean[levels:, :]
        devs = [y - mean for y in x]
        cross = functools.reduce(jnp.add, [y * other_half(y) for y in devs]) * (1.0 / times)
        both = jnp.where(sub < levels, mean * other_half(mean), cross)
        chunks = jnp.concatenate([y * wet for y in x] + [wet, both * wet], axis=0)
        high = chunks.astype(jnp.bfloat16)
        low = (chunks - high.astype(jnp.float32)).astype(jnp.bfloat16)
        iota = lax.broadcasted_iota(jnp.int32, (LANES, LANES), 0)
        tags = jnp.broadcast_to(label[last : last + 1, :], (LANES, LANES))
        hot = jnp.where(tags == iota, 1.0, 0.0).astype(jnp.bfloat16)
        out = lax.dot_general(
            jnp.concatenate([high, low], axis=1),
            jnp.concatenate([hot, hot], axis=1),
            (((1,), (1,)), ((), ())),
            preferred_element_type=jnp.float32,
        )
        out = [out[m * SUB : (m + 1) * SUB, :] for m in range(times + 2)]
        tiles[last * SUB : (last + 1) * SUB, :] = functools.reduce(
            jnp.add, [pltpu.roll(y, BASINS * m, axis=1) if m else y for m, y in enumerate(out)]
        )
        total = functools.reduce(jnp.add, out[:times])
        return in_one_row(jnp.where(sub < levels, out[times], total))

    def other_half(x):
        return pltpu.roll(x, levels, axis=0)

    def over_sublanes(x):
        for shift in (4, 2, 1):
            x = x + pltpu.roll(x, shift, axis=0)
        return x

    def in_one_row(x):
        return over_sublanes(pltpu.roll(x, 0, axis=1, stride=BASINS, stride_axis=0))[0:1, :]

    cuts = (0, steps // 2, steps)
    for low_cut, high_cut in itertools.pairwise(cuts):
        for n in range(low_cut, high_cut):
            if n + 1 < steps:
                warmth_copy(n + 1).wait()
            flow_copy(n).wait()
        for n in range(low_cut, high_cut):
            prepare(n)
            if n:
                contract(n - 1)
    contract(steps - 1)
    pl.semaphore_wait(met_sem, FAN - 1)

    def tile_copy(peer):
        return pltpu.make_async_remote_copy(
            src_ref=tiles.at[pl.ds(pl.multiple_of(peer * SUB, SUB), SUB)],
            dst_ref=tiles_in.at[mine],
            send_sem=tile_send,
            recv_sem=tile_recv,
            device_id=(lat, peer),
            device_id_type=MESH,
        )

    def line_copy(peer):
        return pltpu.make_async_remote_copy(
            src_ref=lines.at[peer],
            dst_ref=lines_in.at[lon],
            send_sem=line_send,
            recv_sem=line_recv,
            device_id=(lat, peer),
            device_id_type=MESH,
        )

    lines_in[pl.ds(lon, 1)] = lines[pl.ds(lon, 1)]
    for copy in (line_copy, tile_copy):
        for peer in map(at, far_first()):

            @pl.when(peer != last)
            def _():
                copy(peer).start()

    @pl.when(lat < lats - 1)
    def _():
        edge_copy.wait_recv()

    @pl.when(lat == lats - 1)
    def _():
        edge_in[...] = jnp.zeros_like(edge_in)

    line = edge_sums()
    edge_line[...] = line
    edge_lines[pl.ds(lon, 1)] = line.reshape(1, 1, LANES)
    for peer in map(at, far_first()):
        pltpu.make_async_remote_copy(
            src_ref=edge_line,
            dst_ref=edge_lines.at[lon],
            send_sem=edge_line_send,
            recv_sem=edge_line_recv,
            device_id=(lat, peer),
            device_id_type=MESH,
        ).start()

    @pl.when(lon != last)
    def _():
        tile_copy(last).start()

    def wait_for(ref, count, send_sem, recv_sem):
        part = pl.ds(0, count)
        return pltpu.make_async_remote_copy(
            src_ref=ref.at[part],
            dst_ref=ref.at[part],
            send_sem=send_sem,
            recv_sem=recv_sem,
            device_id=(lat, lon),
            device_id_type=MESH,
        )

    every_line = wait_for(lines_in, lons - 1, line_send, line_recv)
    fewer_lines = wait_for(lines_in, lons - 2, line_send, line_recv)
    every_edge_line = wait_for(edge_lines, lons - 1, edge_line_send, edge_line_recv)
    every_bar = wait_for(bar_in, lons - 1, bar_send, bar_recv)
    fewer_bars = wait_for(bar_in, lons - 2, bar_send, bar_recv)
    every_tile = wait_for(tiles_in, (lons - 1) * SUB, tile_send, tile_recv)

    def summed(ref):
        total = ref[0:SUB].reshape(SUB, LANES)
        for n in range(1, lons // SUB):
            total = total + ref[n * SUB : (n + 1) * SUB].reshape(SUB, LANES)
        return over_sublanes(total)

    def ratio(total):
        return total / jnp.maximum(pltpu.roll(total, levels * BASINS, axis=1), 1.0)

    @pl.when(lon != last)
    def _():
        every_line.wait_recv()
        line = ratio(summed(lines_in))[0:1, :]
        bar[...] = line
        bar_in[pl.ds(lon, 1)] = line.reshape(1, 1, LANES)
        for peer in map(at, far_first()):
            pltpu.make_async_remote_copy(
                src_ref=bar,
                dst_ref=bar_in.at[lon],
                send_sem=bar_send,
                recv_sem=bar_recv,
                device_id=(lat, peer),
                device_id_type=MESH,
            ).start()

    every_tile.wait_recv()
    parts = [tiles[mine, :]] + [tiles_in[SUB * p : SUB * p + SUB, :] for p in range(lons)]
    while len(parts) > 1:
        parts = [sum(parts[i : i + 2][1:], parts[i]) for i in range(0, len(parts), 2)]
    total = parts[0]

    def moved(x, lanes):
        return pltpu.roll(x, (-lanes) % LANES, axis=1)

    count = moved(total, 10 * times)
    first = lane < BASINS
    divisor = jnp.maximum(count, 1.0)
    sums = total
    for t in range(1, times):
        sums = sums + moved(total, 10 * t)
    bars = jnp.where(first, sums / divisor * (1.0 / times), 0.0)
    bars_w = other_half(bars)
    flow_part = scaling * count * bars * bars_w
    swing = jnp.zeros_like(total)
    for t in range(times):
        dev = (moved(total, 10 * t) if t else total) / divisor - bars
        swing = swing + dev * other_half(dev)
    swing = scaling * count * (swing * (1.0 / times))
    both = moved(total, 10 * (times + 1))
    steady = scaling * both - flow_part
    transient = scaling * other_half(both) - swing
    for q, value in enumerate((flow_part, steady, swing, transient)):
        for k in range(levels):
            transport_ref[q, k] = value[k : k + 1, 0:BASINS]

    every_edge_line.wait_recv()
    last_bars = ratio(summed(edge_lines)) * (1.0 / times)
    @pl.when(lon != last)
    def _():
        fewer_bars.wait_recv()

    @pl.when(lon == last)
    def _():
        every_bar.wait_recv()

    for n in range(steps):
        here = slice(n * SUB, (n + 1) * SUB)
        table = bar_in[here].reshape(SUB, LANES)
        if n == steps - 1:
            table = jnp.where(sub == SUB - 1, last_bars, table)
        lim = limit[here, :]
        tags = label[here, :]
        for k in range(levels):
            cell = jnp.take_along_axis(
                table, tags + (levels * 10 + k * 10), axis=1, mode="promise_in_bounds"
            )
            eddy_ref[k, here, :] = jnp.where(lim > k, mean_warmth[k, here, :] - cell, 0.0)

    every_tile.wait_send()
    every_edge_line.wait_send()

    @pl.when(lon != last)
    def _():
        fewer_lines.wait_send()
        every_bar.wait_send()

    @pl.when(lon == last)
    def _():
        every_line.wait_send()

    @pl.when(lat > 0)
    def _():
        edge_copy.wait_send()


def write_out(eddy, transport, eddy_out, transport_out, sem):
    copies = [
        pltpu.make_async_copy(eddy, eddy_out, sem.at[0]),
        pltpu.make_async_copy(transport, transport_out, sem.at[1]),
    ]
    for copy in copies:
        copy.start()
    for copy in copies:
        copy.wait()


def shards(lats, lons, flow, warmth, flag, floor, label):
    times, levels, rows, cols = flow.shape
    fields = times * levels
    pitch = rows + SUB
    scaling = 1.0 / math.sqrt(cols * lons)
    dims = (times, levels, rows, pitch, lats, lons, scaling)
    local = pl.BlockSpec(memory_space=pltpu.VMEM)
    dma = pltpu.SemaphoreType.DMA
    f32 = jnp.float32
    eddy, transport = pl.pallas_call(
        functools.partial(kernel, dims),
        out_shape=(
            pltpu.VMEM((levels, rows, cols), f32),
            pltpu.VMEM((4, levels, 1, BASINS), f32),
        ),
        in_specs=[pl.BlockSpec(memory_space=pltpu.HBM)] * 5,
        out_specs=(local, local),
        scratch_shapes=[
            pltpu.VMEM((fields, rows, cols), f32),
            pltpu.VMEM((fields, pitch, cols), f32),
            pltpu.VMEM((rows, cols), jnp.int32),
            pltpu.VMEM((rows, cols), jnp.int32),
            pltpu.VMEM((rows, cols), jnp.int32),
            pltpu.VMEM((pitch, cols), jnp.int32),
            pltpu.VMEM((rows, cols), jnp.int32),
            pltpu.VMEM((levels, rows, cols), f32),
            pltpu.VMEM((levels * (2 * times + 4) * SUB, 2 * cols), jnp.bfloat16),
            pltpu.VMEM((levels * (2 * times + 4) * SUB, 2 * cols), jnp.bfloat16),
            pltpu.VMEM((fields + SUB, cols), f32),
            pltpu.VMEM((fields + SUB, cols), f32),
            pltpu.VMEM((rows * SUB, cols), f32),
            pltpu.VMEM((rows * SUB, cols), f32),
            pltpu.VMEM((1, cols), f32),
            pltpu.VMEM((rows, 1, cols), f32),
            pltpu.VMEM((1, cols), f32),
            pltpu.VMEM((rows, 1, cols), f32),
            pltpu.VMEM((rows, 1, cols), f32),
            pltpu.VMEM((rows, 1, cols), f32),
            dma((rows // SUB,)),
            dma((rows // SUB,)),
            dma((3,)),
            dma,
            dma,
            dma,
            dma,
            dma,
            dma,
            dma,
            dma,
            dma,
            dma,
            pltpu.SemaphoreType.REGULAR,
        ],
        compiler_params=pltpu.CompilerParams(
            collective_id=0, has_side_effects=True, vmem_limit_bytes=66879488
        ),
    )(
        flow.reshape(fields, rows, cols),
        warmth.reshape(fields, rows, cols),
        flag,
        floor,
        label,
    )
    eddy, transport = pl.pallas_call(
        write_out,
        out_shape=tuple(jax.ShapeDtypeStruct(a.shape, a.dtype) for a in (eddy, transport)),
        in_specs=[local] * 2,
        out_specs=[pl.BlockSpec(memory_space=pltpu.HBM)] * 2,
        scratch_shapes=[dma((2,))],
        compiler_params=pltpu.CompilerParams(vmem_limit_bytes=2**20),
    )(eddy, transport)
    return eddy, jnp.transpose(transport, (0, 3, 1, 2))


def solution(mesh):
    return jax.shard_map(
        functools.partial(shards, mesh.shape["lat"], mesh.shape["lon"]),
        mesh=mesh,
        in_specs=(
            P(None, None, "lat", "lon"),
            P(None, None, "lat", "lon"),
            P("lat", "lon"),
            P("lat", "lon"),
            P("lat", "lon"),
        ),
        out_specs=(P(None, "lat", "lon"), P(None, None, None, ("lat", "lon"))),
        check_vma=False,
    )
```

```python
import functools
import itertools
import math

import jax
import jax.numpy as jnp
from jax import lax
from jax.experimental import pallas as pl
from jax.experimental.pallas import tpu as pltpu
from jax.sharding import PartitionSpec as P

BASINS = 10
OWNER_PART = 4
CORES = 2
FAN = 4
GROUP = 16
SUB = 8
LANES = 128
MESH = pl.DeviceIdType.MESH


def kernel(
    dims,
    flow_hbm,
    warmth_hbm,
    flag_hbm,
    floor_hbm,
    label_hbm,
    eddy_ref,
    transport_ref,
    flow,
    warmth,
    flag,
    floor,
    label,
    depth,
    limit,
    mean_warmth,
    sums,
    split_even,
    split_odd,
    edge,
    edge_in,
    edge_sum,
    edge_sum_in,
    tiles,
    tiles_in,
    bar,
    bar_in,
    edge_line,
    edge_lines,
    lines,
    lines_in,
    tiles_near,
    tiles_last,
    last_tile,
    own_total,
    flow_sem,
    warmth_sem,
    small_sem,
    edge_send,
    edge_recv,
    edge_sum_send,
    edge_sum_recv,
    near_send,
    near_recv,
    last_send,
    last_recv,
    tile_send,
    tile_recv,
    bar_send,
    bar_recv,
    line_send,
    line_recv,
    edge_line_send,
    edge_line_recv,
    met_sem,
):
    splits = (split_even, split_odd)
    times, levels, rows, pitch, lats, lons, owners, share, scaling = dims
    steps = rows // SUB
    lat, lon = lax.axis_index("lat"), lax.axis_index("lon")
    fields = times * levels
    last = rows - 1
    mine = pl.ds(pl.multiple_of(lon * SUB, SUB), SUB)
    places = round(math.log(lons, FAN))
    flat_flow = flow.reshape(fields * rows, LANES)
    flat_sums = sums.reshape(levels * pitch, LANES)
    flat_mean = mean_warmth.reshape(levels * rows, LANES)
    flat_warmth = warmth.reshape(fields * pitch, LANES)

    def flow_copy(n):
        part = pl.ds(pl.multiple_of(n * SUB, SUB), SUB)
        return pltpu.make_async_copy(flow_hbm.at[:, part], flow.at[:, part], flow_sem.at[n])

    def warmth_copy(n):
        part = pl.ds(pl.multiple_of(n * SUB, SUB), SUB)
        return pltpu.make_async_copy(warmth_hbm.at[:, part], warmth.at[:, part], warmth_sem.at[n])

    smalls = [
        pltpu.make_async_copy(flag_hbm, flag, small_sem.at[0]),
        pltpu.make_async_copy(floor_hbm, floor, small_sem.at[1]),
        pltpu.make_async_copy(label_hbm, label, small_sem.at[2]),
    ]
    warmth_copy(0).start()
    for copy in smalls:
        copy.start()

    barrier = pltpu.get_barrier_semaphore()
    turned_digits = [
        [lax.rem(lon // FAN**d + i, FAN) * FAN**d for i in range(FAN)] for d in range(places)
    ]
    is_owner = lon < owners

    def far_first():
        ways = itertools.product(range(FAN), repeat=places)
        hops = lambda way: sum(min(i, FAN - i) for i in way[1:]) + (way[0] > 0)
        return [way for way in sorted(ways, key=hops, reverse=True) if any(way)]

    def at(way):
        return sum(turned_digits[d][way[d]] for d in range(places))

    def signal(semaphore, way):
        pl.semaphore_signal(semaphore, inc=1, device_id=(lat, at(way)), device_id_type=MESH)

    def line_ways(d):
        return [way for way in far_first() if way[d] and sum(i > 0 for i in way) == 1]

    @pl.when(is_owner)
    def _():
        for way in far_first():
            signal(barrier, way)

    @pl.when(jnp.logical_not(is_owner))
    def _():
        for d in range(places):
            for way in line_ways(d):
                signal(barrier, way)

    @pl.when(lat < lats - 1)
    def _():
        pl.semaphore_signal(barrier, inc=1, device_id=(lat + 1, lon), device_id_type=MESH)

    for n in range(1, steps):
        warmth_copy(n).start()
    for a in range(fields // SUB):
        flat_warmth[pl.ds(a * SUB * pitch + rows, SUB, stride=pitch), :] = jnp.zeros(
            (SUB, LANES), jnp.float32
        )
    for k in range(levels):
        flat_sums[k * pitch + rows : k * pitch + rows + SUB, :] = jnp.zeros(
            (SUB, LANES), jnp.float32
        )
    depth[rows : rows + SUB, :] = jnp.zeros((SUB, LANES), jnp.int32)
    own_chip = pl.ds(pl.multiple_of(lon // CORES * SUB, SUB), SUB)
    tiles_in[own_chip, :] = jnp.zeros((SUB, LANES), jnp.float32)
    for copy in smalls:
        copy.wait()
    warmth_copy(0).wait()
    for n in range(steps):
        flow_copy(n).start()
    depth[0:rows, :] = flag[...] * floor[...]
    lane = lax.broadcasted_iota(jnp.int32, (SUB, LANES), 1)
    sub = lax.broadcasted_iota(jnp.int32, (SUB, LANES), 0)
    slots = times + 2
    turned = (lane + GROUP * sub) % LANES
    marks = [(turned >= BASINS * m) & (turned < BASINS * (m + 1)) for m in range(slots)]

    def two_parts(x):
        high = x.astype(jnp.bfloat16)
        return high, (x - high.astype(jnp.float32)).astype(jnp.bfloat16)

    def straight(x):
        return pltpu.roll(x, 0, axis=1, stride=GROUP, stride_axis=0)

    def hot_rows(n):
        iota = lax.broadcasted_iota(jnp.int32, (GROUP, LANES), 0)
        tags = label[n * SUB : (n + 1) * SUB, :]
        hot = jnp.concatenate(
            [
                jnp.where(
                    jnp.broadcast_to(tags[r : r + 1, :], (GROUP, LANES)) == iota, 1.0, 0.0
                )
                for r in (0, *range(SUB - 1, 0, -1))
            ],
            axis=0,
        ).astype(jnp.bfloat16)
        return jnp.concatenate([hot, hot], axis=1)

    def summed_over(data, hot):
        return lax.dot_general(
            data, hot, (((1,), (1,)), ((), ())), preferred_element_type=jnp.float32
        )

    def piece(out, c, m):
        x = out[c * SUB : (c + 1) * SUB, :]
        return pltpu.roll(x, BASINS * m, axis=1) if m else x

    def sum_times(n):
        here = pl.ds(n * SUB, SUB)
        for k in range(levels):
            sums[k, here, :] = functools.reduce(
                jnp.add, [warmth[t * levels + k, here, :] for t in range(times)]
            )

    for n in range(1, steps):
        warmth_copy(n).wait()
    for n in range(steps):
        sum_times(n)
    for n in range(steps):
        here = pl.ds(n * SUB, SUB)
        lim = jnp.minimum(depth[here, :], depth[pl.ds(n * SUB + 1, SUB), :])
        limit[here, :] = lim
        chunks = []
        for k in range(levels):
            wet = jnp.where(lim > k, 1.0, 0.0)
            mean_w = (sums[k, here, :] + flat_sums[pl.ds(k * pitch + n * SUB + 1, SUB), :]) * (
                0.5 / times
            )
            mean_warmth[k, here, :] = mean_w
            chunks += [wet, mean_w * wet]
        data = jnp.concatenate(two_parts(jnp.concatenate(chunks, axis=0)), axis=1)
        out = summed_over(data, hot_rows(n))
        line = jnp.zeros((SUB, LANES), jnp.float32)
        for k in range(levels):
            line = jnp.where(marks[k], piece(out, 2 * k, k), line)
            line = jnp.where(marks[levels + k], piece(out, 2 * k + 1, levels + k), line)
        line = straight(line)
        lines[n * SUB // share : (n + 1) * SUB // share] = line.reshape(
            SUB // share, share, LANES
        )

    edge_sum[...] = jnp.concatenate(
        [flat_sums[pl.ds(0, levels, stride=pitch), :], depth[0:levels, :].astype(jnp.float32)],
        axis=0,
    )
    edge_sum_copy = pltpu.make_async_remote_copy(
        src_ref=edge_sum,
        dst_ref=edge_sum_in,
        send_sem=edge_sum_send,
        recv_sem=edge_sum_recv,
        device_id=(lat - 1, lon),
        device_id_type=MESH,
    )
    edge_copy = pltpu.make_async_remote_copy(
        src_ref=edge,
        dst_ref=edge_in,
        send_sem=edge_send,
        recv_sem=edge_recv,
        device_id=(lat - 1, lon),
        device_id_type=MESH,
    )
    owner_slots = owners // FAN ** (places - 1)
    met = jnp.where(
        is_owner,
        owners - 1 + FAN - owner_slots,
        owners + (places - 1) * (FAN - 1) + FAN - 1 - owner_slots,
    )
    pl.semaphore_wait(barrier, jnp.where(lat > 0, met + 1, met))

    @pl.when(lat > 0)
    def _():
        edge_sum_copy.start()

    for way in line_ways(1):
        signal(met_sem.at[0], way)

    def to_device(src, dst, send_sem, recv_sem, device):
        return pltpu.make_async_remote_copy(
            src_ref=src,
            dst_ref=dst,
            send_sem=send_sem,
            recv_sem=recv_sem,
            device_id=(lat, device),
            device_id_type=MESH,
        )

    inner = FAN ** (places - 1)
    for way in [*far_first(), (0,) * places]:
        if way[-1] == 0:
            for first_digit in range(owner_slots):
                owner = at(way) - turned_digits[-1][0] + first_digit * inner

                def start(owner=owner):
                    to_device(
                        lines.at[owner], lines_in.at[lon], line_send, line_recv, owner
                    ).start()

                if any(way):
                    start()
                else:
                    pl.when(owner != lon)(start)

    @pl.when(is_owner)
    def _():
        lines_in[pl.ds(lon, 1)] = lines[pl.ds(lon, 1)]

    for a in range(fields // SUB):
        edge[a * SUB : (a + 1) * SUB, :] = flat_warmth[pl.ds(a * SUB * pitch, SUB, stride=pitch), :]

    @pl.when(lat > 0)
    def _():
        edge_copy.start()

    width = 2 * times + 4

    def prepare(n):
        row = n * SUB
        here = pl.ds(row, SUB)
        split = splits[n % 2]
        lim = limit[here, :]
        for k in range(levels):
            wet = jnp.where(lim > k, 1.0, 0.0)
            v = [flow[t * levels + k, here, :] for t in range(times)]
            w = [
                0.5
                * (
                    warmth[t * levels + k, here, :]
                    + flat_warmth[pl.ds((t * levels + k) * pitch + row + 1, SUB), :]
                )
                for t in range(times)
            ]
            mean_v = functools.reduce(jnp.add, v) * (1.0 / times)
            mean_w = mean_warmth[k, here, :]
            cross = functools.reduce(
                jnp.add, [(v[t] - mean_v) * (w[t] - mean_w) for t in range(times)]
            ) * (1.0 / times)
            chunks = [x * wet for x in v] + [x * wet for x in w]
            chunks += [wet, mean_v * mean_w * wet, cross * wet, jnp.zeros_like(wet)]
            for c in range(0, width, 2):
                high, low = two_parts(jnp.concatenate(chunks[c : c + 2], axis=0))
                at_row = (k * width + c) * SUB
                split[at_row : at_row + 2 * SUB, 0:LANES] = high
                split[at_row : at_row + 2 * SUB, LANES : 2 * LANES] = low

    def contract(n):
        out = summed_over(splits[n % 2][...], hot_rows(n))
        for k in range(levels):
            count = piece(out, k * width + 2 * times, times)
            for half in range(2):
                acc = jnp.where(marks[times], count, 0.0)
                for t in range(times):
                    acc = jnp.where(marks[t], piece(out, k * width + half * times + t, t), acc)
                both = piece(out, k * width + 2 * times + 1 + half, times + 1)
                acc = jnp.where(marks[times + 1], both, acc)
                tiles[pl.ds(n * SUB * SUB + half * levels + k, SUB, stride=SUB), :] = straight(acc)

    def last_hot(size):
        iota = lax.broadcasted_iota(jnp.int32, (size, LANES), 0)
        tags = jnp.broadcast_to(label[last : last + 1, :], (size, LANES))
        hot = jnp.where(tags == iota, 1.0, 0.0).astype(jnp.bfloat16)
        return jnp.concatenate([hot, hot], axis=1)

    def edge_line_of_sums():
        lim = jnp.minimum(
            depth[last : last + 1, :], edge_sum_in[levels : levels + 1, :].astype(jnp.int32)
        )
        limit[last : last + 1, :] = lim
        wet = jnp.where(jnp.broadcast_to(lim, (SUB, LANES)) > sub % levels, 1.0, 0.0)
        here = flat_sums[pl.ds(last, levels, stride=pitch), :]
        mean = (here + edge_sum_in[0:levels, :]) * (0.5 / times)
        flat_mean[pl.ds(last, levels, stride=rows), :] = mean
        chunk = wet * jnp.concatenate([jnp.ones_like(mean), mean], axis=0)
        data = jnp.concatenate(two_parts(jnp.concatenate([chunk] * 2, axis=0)), axis=1)
        return in_one_row(summed_over(data, last_hot(LANES))[0:SUB, :])

    def edge_tile():
        lim = limit[last : last + 1, :]
        wet = jnp.where(jnp.broadcast_to(lim, (SUB, LANES)) > sub % levels, 1.0, 0.0)
        x = []
        for t in range(times):
            v = flat_flow[pl.ds(t * levels * rows + last, levels, stride=rows), :]
            w = flat_warmth[pl.ds(t * levels * pitch + last, levels, stride=pitch), :]
            w = 0.5 * (w + edge_in[t * levels : (t + 1) * levels, :])
            x.append(jnp.concatenate([v, w], axis=0))
        mean = functools.reduce(jnp.add, x) * (1.0 / times)
        devs = [y - mean for y in x]
        cross = functools.reduce(jnp.add, [y * other_half(y) for y in devs]) * (1.0 / times)
        both = jnp.where(sub < levels, mean * other_half(mean), cross)
        chunks = jnp.concatenate([y * wet for y in x] + [wet, both * wet], axis=0)
        data = jnp.concatenate(two_parts(chunks), axis=1)
        out = summed_over(data, last_hot(LANES))
        return functools.reduce(jnp.add, [piece(out, m, m) for m in range(slots)])

    def other_half(x):
        return pltpu.roll(x, levels, axis=0)

    def over_sublanes(x):
        for shift in (4, 2, 1):
            x = x + pltpu.roll(x, shift, axis=0)
        return x

    def in_one_row(x):
        return over_sublanes(pltpu.roll(x, 0, axis=1, stride=BASINS, stride_axis=0))[0:1, :]

    def wait_for(ref, count, send_sem, recv_sem):
        part = pl.ds(0, count)
        return pltpu.make_async_remote_copy(
            src_ref=ref.at[part],
            dst_ref=ref.at[part],
            send_sem=send_sem,
            recv_sem=recv_sem,
            device_id=(lat, lon),
            device_id_type=MESH,
        )

    cuts = (0, steps // 2, steps)
    for low_cut, high_cut in itertools.pairwise(cuts):
        for n in range(low_cut, high_cut):
            flow_copy(n).wait()
        for n in range(low_cut, high_cut):
            prepare(n)
            if n:
                contract(n - 1)
        if high_cut < steps:
            pl.semaphore_wait(met_sem.at[0], FAN - 1)
            for way in line_ways(places - 1):
                signal(met_sem.at[1], way)
    contract(steps - 1)
    core = lax.rem(lon, CORES)
    partner = lon + 1 - CORES * core

    def tile(ref, row):
        return ref.at[pl.ds(pl.multiple_of(row * SUB, SUB), SUB)]

    pairs = rows // CORES
    for i in range(pairs):
        to_device(
            tile(tiles, CORES * i + 1 - core), tile(tiles_near, i), near_send, near_recv, partner
        ).start()

    every_line = wait_for(lines_in, lons - 1, line_send, line_recv)
    sent_lines = wait_for(lines, owners, line_send, line_recv)
    fewer_sent_lines = wait_for(lines, owners - 1, line_send, line_recv)
    sent_bars = wait_for(lines_in, lons - 1, bar_send, bar_recv)
    every_bar = wait_for(bar_in, owners, bar_send, bar_recv)
    fewer_bars = wait_for(bar_in, owners - 1, bar_send, bar_recv)
    every_edge_line = wait_for(edge_lines, lons - 1, edge_line_send, edge_line_recv)
    every_near = wait_for(tiles_near, pairs * SUB, near_send, near_recv)
    every_tile = wait_for(tiles_in, (pairs - 1) * SUB, tile_send, tile_recv)
    fewer_tiles = wait_for(tiles_in, (pairs - 2) * SUB, tile_send, tile_recv)
    every_last = wait_for(tiles_last, (lons - 1) * SUB, last_send, last_recv)

    def tree_sum(parts):
        while len(parts) > 1:
            parts = [sum(parts[i : i + 2][1:], parts[i]) for i in range(0, len(parts), 2)]
        return parts[0]

    def ratio(total):
        return total / jnp.maximum(pltpu.roll(total, levels * BASINS, axis=1), 1.0)

    pl.semaphore_wait(met_sem.at[1], FAN - 1)

    every_near.wait_recv()
    for i in range(pairs):
        own = pl.ds(pl.multiple_of((CORES * i + core) * SUB, SUB), SUB)
        tiles[own, :] = tiles[own, :] + tiles_near[i * SUB : (i + 1) * SUB, :]
    for way in far_first():
        if way[0] % CORES == 0:
            peer = at(way)

            @pl.when(peer != last)
            def _():
                to_device(
                    tile(tiles, peer), tile(tiles_in, lon // CORES), tile_send, tile_recv, peer
                ).start()

    @pl.when(lat < lats - 1)
    def _():
        edge_sum_copy.wait_recv()

    @pl.when(lat == lats - 1)
    def _():
        edge_sum_in[...] = jnp.zeros_like(edge_sum_in)

    line = edge_line_of_sums()
    edge_line[...] = line
    edge_lines[pl.ds(lon, 1)] = line.reshape(1, 1, LANES)
    for peer in map(at, far_first()):
        to_device(edge_line, edge_lines.at[lon], edge_line_send, edge_line_recv, peer).start()

    @pl.when(is_owner)
    def _():
        every_line.wait_recv()
        bar[...] = ratio(tree_sum([lines_in[p] for p in range(lons)]))
        bar_in[pl.ds(lon, 1)] = bar[...][None]
        for peer in map(at, far_first()):
            to_device(bar, bar_in.at[lon], bar_send, bar_recv, peer).start()

    @pl.when(lat < lats - 1)
    def _():
        edge_copy.wait_recv()

    @pl.when(lat == lats - 1)
    def _():
        edge_in[...] = jnp.zeros_like(edge_in)

    last_tile[...] = edge_tile()
    tiles_last[mine, :] = last_tile[...]

    @pl.when(lon != last)
    def _():
        to_device(last_tile, tile(tiles_last, lon), last_send, last_recv, last).start()

    def tiles_of(ref, count):
        return [ref[SUB * p : SUB * (p + 1), :] for p in range(count)]

    @pl.when(lon != last)
    def _():
        every_tile.wait_recv()
        own_total[...] = tree_sum([tiles[mine, :], *tiles_of(tiles_in, pairs)])

    @pl.when(lon == last)
    def _():
        every_last.wait_recv()
        own_total[...] = tree_sum(tiles_of(tiles_last, lons))

    total = own_total[...]

    def moved(x, lanes):
        return pltpu.roll(x, (-lanes) % LANES, axis=1)

    count = moved(total, BASINS * times)
    first = lane < BASINS
    divisor = jnp.maximum(count, 1.0)
    time_sums = total
    for t in range(1, times):
        time_sums = time_sums + moved(total, BASINS * t)
    bars = jnp.where(first, time_sums / divisor * (1.0 / times), 0.0)

    bars_w = other_half(bars)
    flow_part = scaling * count * bars * bars_w
    swing = jnp.zeros_like(total)
    for t in range(times):
        dev = (moved(total, 10 * t) if t else total) / divisor - bars
        swing = swing + dev * other_half(dev)
    swing = scaling * count * (swing * (1.0 / times))
    both = moved(total, 10 * (times + 1))
    steady = scaling * both - flow_part
    transient = scaling * other_half(both) - swing
    for q, value in enumerate((flow_part, steady, swing, transient)):
        for k in range(levels):
            transport_ref[q, k] = value[k : k + 1, 0:BASINS]

    every_edge_line.wait_recv()
    total = edge_lines[0:SUB].reshape(SUB, LANES)
    for n in range(1, steps):
        total = total + edge_lines[n * SUB : (n + 1) * SUB].reshape(SUB, LANES)
    last_bars = ratio(over_sublanes(total))
    @pl.when(is_owner)
    def _():
        fewer_bars.wait_recv()

    @pl.when(jnp.logical_not(is_owner))
    def _():
        every_bar.wait_recv()

    for n in range(steps):
        here = slice(n * SUB, (n + 1) * SUB)
        table = bar_in[n * SUB // share : (n + 1) * SUB // share].reshape(SUB, LANES)
        if n == steps - 1:
            table = jnp.where(sub == SUB - 1, last_bars, table)
        lim = limit[here, :]
        tags = label[here, :]
        for k in range(levels):
            cell = jnp.take_along_axis(
                table, tags + (levels + k) * BASINS, axis=1, mode="promise_in_bounds"
            )
            eddy_ref[k, here, :] = jnp.where(lim > k, mean_warmth[k, here, :] - cell, 0.0)

    for copies in (every_near, every_edge_line):
        copies.wait_send()

    @pl.when(is_owner)
    def _():
        fewer_sent_lines.wait_send()
        sent_bars.wait_send()

    @pl.when(jnp.logical_not(is_owner))
    def _():
        sent_lines.wait_send()

    skips_last = (core == CORES - 1) & (lon != last)

    @pl.when(skips_last)
    def _():
        fewer_tiles.wait_send()

    @pl.when(jnp.logical_not(skips_last))
    def _():
        every_tile.wait_send()

    @pl.when(lon != last)
    def _():
        wait_for(last_tile, SUB, last_send, last_recv).wait_send()

    @pl.when(lat > 0)
    def _():
        edge_copy.wait_send()
        edge_sum_copy.wait_send()


def write_out(eddy, transport, eddy_out, transport_out, sem):
    copies = [
        pltpu.make_async_copy(eddy, eddy_out, sem.at[0]),
        pltpu.make_async_copy(transport, transport_out, sem.at[1]),
    ]
    for copy in copies:
        copy.start()
    for copy in copies:
        copy.wait()


def shards(lats, lons, flow, warmth, flag, floor, label):
    times, levels, rows, cols = flow.shape
    fields = times * levels
    pitch = rows + SUB
    scaling = 1.0 / math.sqrt(cols * lons)
    owners = lons // OWNER_PART
    share = rows // owners
    dims = (times, levels, rows, pitch, lats, lons, owners, share, scaling)
    local = pl.BlockSpec(memory_space=pltpu.VMEM)
    dma = pltpu.SemaphoreType.DMA
    f32 = jnp.float32
    eddy, transport = pl.pallas_call(
        functools.partial(kernel, dims),
        out_shape=(
            pltpu.VMEM((levels, rows, cols), f32),
            pltpu.VMEM((4, levels, 1, BASINS), f32),
        ),
        in_specs=[pl.BlockSpec(memory_space=pltpu.HBM)] * 5,
        out_specs=(local, local),
        scratch_shapes=[
            pltpu.VMEM((fields, rows, cols), f32),
            pltpu.VMEM((fields, pitch, cols), f32),
            pltpu.VMEM((rows, cols), jnp.int32),
            pltpu.VMEM((rows, cols), jnp.int32),
            pltpu.VMEM((rows, cols), jnp.int32),
            pltpu.VMEM((pitch, cols), jnp.int32),
            pltpu.VMEM((rows, cols), jnp.int32),
            pltpu.VMEM((levels, rows, cols), f32),
            pltpu.VMEM((levels, pitch, cols), f32),
            pltpu.VMEM((levels * (2 * times + 4) * SUB, 2 * cols), jnp.bfloat16),
            pltpu.VMEM((levels * (2 * times + 4) * SUB, 2 * cols), jnp.bfloat16),
            pltpu.VMEM((fields, cols), f32),
            pltpu.VMEM((fields, cols), f32),
            pltpu.VMEM((2 * levels, cols), f32),
            pltpu.VMEM((2 * levels, cols), f32),
            pltpu.VMEM((rows * SUB, cols), f32),
            pltpu.VMEM((rows // CORES * SUB, cols), f32),
            pltpu.VMEM((share, cols), f32),
            pltpu.VMEM((owners, share, cols), f32),
            pltpu.VMEM((1, cols), f32),
            pltpu.VMEM((rows, 1, cols), f32),
            pltpu.VMEM((owners, share, cols), f32),
            pltpu.VMEM((lons, share, cols), f32),
            pltpu.VMEM((rows // CORES * SUB, cols), f32),
            pltpu.VMEM((rows * SUB, cols), f32),
            pltpu.VMEM((SUB, cols), f32),
            pltpu.VMEM((SUB, cols), f32),
            dma((rows // SUB,)),
            dma((rows // SUB,)),
            dma((3,)),
        ]
        + [dma] * 16
        + [
            pltpu.SemaphoreType.REGULAR((2,)),
        ],
        compiler_params=pltpu.CompilerParams(
            collective_id=0, has_side_effects=True, vmem_limit_bytes=66879488
        ),
    )(
        flow.reshape(fields, rows, cols),
        warmth.reshape(fields, rows, cols),
        flag,
        floor,
        label,
    )
    eddy, transport = pl.pallas_call(
        write_out,
        out_shape=tuple(jax.ShapeDtypeStruct(a.shape, a.dtype) for a in (eddy, transport)),
        in_specs=[local] * 2,
        out_specs=[pl.BlockSpec(memory_space=pltpu.HBM)] * 2,
        scratch_shapes=[dma((2,))],
        compiler_params=pltpu.CompilerParams(vmem_limit_bytes=2**20),
    )(eddy, transport)
    return eddy, jnp.transpose(transport, (0, 3, 1, 2))


def solution(mesh):
    return jax.shard_map(
        functools.partial(shards, mesh.shape["lat"], mesh.shape["lon"]),
        mesh=mesh,
        in_specs=(
            P(None, None, "lat", "lon"),
            P(None, None, "lat", "lon"),
            P("lat", "lon"),
            P("lat", "lon"),
            P("lat", "lon"),
        ),
        out_specs=(P(None, "lat", "lon"), P(None, None, None, ("lat", "lon"))),
        check_vma=False,
    )
```

```python
import functools
import itertools
import math

import jax
import jax.numpy as jnp
from jax import lax
from jax.experimental import pallas as pl
from jax.experimental.pallas import tpu as pltpu
from jax.sharding import PartitionSpec as P

BASINS = 10
OWNER_PART = 8
CORES = 2
FAN = 4
GROUP = 16
SUB = 8
LANES = 128
MESH = pl.DeviceIdType.MESH


def kernel(
    dims,
    flow_hbm,
    warmth_hbm,
    flag_hbm,
    floor_hbm,
    label_hbm,
    eddy_ref,
    transport_ref,
    flow,
    warmth,
    flag,
    floor,
    label,
    depth,
    limit,
    mean_warmth,
    sums,
    split_even,
    split_odd,
    edge,
    edge_in,
    edge_sum,
    edge_sum_in,
    tiles,
    tiles_in,
    bar,
    bar_in,
    edge_line,
    edge_lines,
    lines,
    lines_in,
    tiles_near,
    tiles_last,
    last_tile,
    own_total,
    flow_sem,
    warmth_sem,
    small_sem,
    edge_send,
    edge_recv,
    edge_sum_recv,
    near_recv,
    tile_recv,
    bar_recv,
    line_recv,
    edge_line_send,
    edge_line_recv,
    sum_send,
    mean_send,
    met_sem,
):
    splits = (split_even, split_odd)
    times, levels, rows, pitch, lats, lons, owners, share, scaling = dims
    steps = rows // SUB
    lat, lon = lax.axis_index("lat"), lax.axis_index("lon")
    fields = times * levels
    last = rows - 1
    mine = pl.ds(pl.multiple_of(lon * SUB, SUB), SUB)
    places = round(math.log(lons, FAN))
    flat_flow = flow.reshape(fields * rows, LANES)
    flat_sums = sums.reshape(levels * pitch, LANES)
    flat_mean = mean_warmth.reshape(levels * rows, LANES)
    flat_warmth = warmth.reshape(fields * pitch, LANES)

    def flow_copy(n):
        part = pl.ds(pl.multiple_of(n * SUB, SUB), SUB)
        return pltpu.make_async_copy(flow_hbm.at[:, part], flow.at[:, part], flow_sem.at[2 * n // steps])

    def warmth_copy(n):
        part = pl.ds(pl.multiple_of(n * SUB, SUB), SUB)
        return pltpu.make_async_copy(warmth_hbm.at[:, part], warmth.at[:, part], warmth_sem.at[min(n, 1) + 2 * n // steps])

    smalls = [
        pltpu.make_async_copy(flag_hbm, flag, small_sem),
        pltpu.make_async_copy(floor_hbm, floor, small_sem),
        pltpu.make_async_copy(label_hbm, label, small_sem),
    ]

    def wait_rows(source, target, first, end, sem):
        part = pl.ds(first * SUB, (end - first) * SUB)
        pltpu.make_async_copy(source.at[:, part], target.at[:, part], sem).wait()

    warmth_copy(0).start()
    for copy in smalls:
        copy.start()

    barrier = pltpu.get_barrier_semaphore()
    turned_digits = [
        [lax.rem(lon // FAN**d + i, FAN) * FAN**d for i in range(FAN)] for d in range(places)
    ]
    reach = owners * CORES

    def owns(device):
        return (device < reach) & (lax.rem(device, CORES) == CORES - 1)

    is_owner = owns(lon)

    def far_first():
        ways = itertools.product(range(FAN), repeat=places)
        hops = lambda way: sum(min(i, FAN - i) for i in way[1:]) + (way[0] > 0)
        return [way for way in sorted(ways, key=hops, reverse=True) if any(way)]

    def at(way):
        return sum(turned_digits[d][way[d]] for d in range(places))

    def signal(semaphore, way):
        pl.semaphore_signal(semaphore, inc=1, device_id=(lat, at(way)), device_id_type=MESH)

    def line_ways(d):
        return [way for way in far_first() if way[d] and sum(i > 0 for i in way) == 1]

    @pl.when(is_owner)
    def _():
        for way in far_first():
            signal(barrier, way)

    @pl.when(jnp.logical_not(is_owner))
    def _():
        for d in range(places):
            for way in line_ways(d):
                signal(barrier, way)

    @pl.when(lat < lats - 1)
    def _():
        pl.semaphore_signal(barrier, inc=1, device_id=(lat + 1, lon), device_id_type=MESH)

    for n in range(1, steps):
        warmth_copy(n).start()
    for a in range(fields // SUB):
        flat_warmth[pl.ds(a * SUB * pitch + rows, SUB, stride=pitch), :] = jnp.zeros(
            (SUB, LANES), jnp.float32
        )
    for k in range(levels):
        flat_sums[k * pitch + rows : k * pitch + rows + SUB, :] = jnp.zeros(
            (SUB, LANES), jnp.float32
        )
    depth[rows : rows + SUB, :] = jnp.zeros((SUB, LANES), jnp.int32)
    own_chip = pl.ds(pl.multiple_of(lon // CORES * SUB, SUB), SUB)
    tiles_in[own_chip, :] = jnp.zeros((SUB, LANES), jnp.float32)
    pltpu.make_async_copy(
        flow_hbm.at[0 : len(smalls)], flow.at[0 : len(smalls)], small_sem
    ).wait()
    warmth_copy(0).wait()
    for n in range(steps):
        flow_copy(n).start()
    depth[0:rows, :] = flag[...] * floor[...]
    lane = lax.broadcasted_iota(jnp.int32, (SUB, LANES), 1)
    sub = lax.broadcasted_iota(jnp.int32, (SUB, LANES), 0)
    slots = times + 2
    turned = (lane + GROUP * sub) % LANES
    marks = [(turned >= BASINS * m) & (turned < BASINS * (m + 1)) for m in range(slots)]

    def two_parts(x):
        high = x.astype(jnp.bfloat16)
        return high, (x - high.astype(jnp.float32)).astype(jnp.bfloat16)

    def straight(x):
        return pltpu.roll(x, 0, axis=1, stride=GROUP, stride_axis=0)

    def hot_rows(n):
        iota = lax.broadcasted_iota(jnp.int32, (GROUP, LANES), 0)
        tags = label[n * SUB : (n + 1) * SUB, :]
        hot = jnp.concatenate(
            [
                jnp.where(
                    jnp.broadcast_to(tags[r : r + 1, :], (GROUP, LANES)) == iota, 1.0, 0.0
                )
                for r in (0, *range(SUB - 1, 0, -1))
            ],
            axis=0,
        ).astype(jnp.bfloat16)
        return jnp.concatenate([hot, hot], axis=1)

    def summed_over(data, hot):
        return lax.dot_general(
            data, hot, (((1,), (1,)), ((), ())), preferred_element_type=jnp.float32
        )

    def piece(out, c, m):
        x = out[c * SUB : (c + 1) * SUB, :]
        return pltpu.roll(x, BASINS * m, axis=1) if m else x

    def sum_times(n):
        here = pl.ds(n * SUB, SUB)
        for k in range(levels):
            sums[k, here, :] = functools.reduce(
                jnp.add, [warmth[t * levels + k, here, :] for t in range(times)]
            )

    wait_rows(warmth_hbm, warmth, 1, steps // 2, warmth_sem.at[1])
    for n in range(steps // 2):
        sum_times(n)
    wait_rows(warmth_hbm, warmth, steps // 2, steps, warmth_sem.at[2])
    for n in range(steps // 2, steps):
        sum_times(n)
    for n in range(steps):
        here = pl.ds(n * SUB, SUB)
        lim = jnp.minimum(depth[here, :], depth[pl.ds(n * SUB + 1, SUB), :])
        limit[here, :] = lim
        chunks = []
        for k in range(levels):
            wet = jnp.where(lim > k, 1.0, 0.0)
            mean_w = (sums[k, here, :] + flat_sums[pl.ds(k * pitch + n * SUB + 1, SUB), :]) * (
                0.5 / times
            )
            mean_warmth[k, here, :] = mean_w
            chunks += [wet, mean_w * wet]
        data = jnp.concatenate(two_parts(jnp.concatenate(chunks, axis=0)), axis=0)
        out = summed_over(data, hot_rows(n)[:, 0:LANES])
        out = out[0 : 2 * levels * SUB, :] + out[2 * levels * SUB :, :]
        line = jnp.zeros((SUB, LANES), jnp.float32)
        for k in range(levels):
            line = jnp.where(marks[k], piece(out, 2 * k, k), line)
            line = jnp.where(marks[levels + k], piece(out, 2 * k + 1, levels + k), line)
        line = straight(line)
        lines[n * SUB // share : (n + 1) * SUB // share] = line.reshape(
            SUB // share, share, LANES
        )

    edge_sum[...] = jnp.concatenate(
        [flat_sums[pl.ds(0, levels, stride=pitch), :], depth[0:levels, :].astype(jnp.float32)],
        axis=0,
    )
    edge_sum_copy = pltpu.make_async_remote_copy(
        src_ref=edge_sum,
        dst_ref=edge_sum_in,
        send_sem=edge_send,
        recv_sem=edge_sum_recv,
        device_id=(lat - 1, lon),
        device_id_type=MESH,
    )
    edge_copy = pltpu.make_async_remote_copy(
        src_ref=edge,
        dst_ref=edge_in,
        send_sem=edge_send,
        recv_sem=edge_recv,
        device_id=(lat - 1, lon),
        device_id_type=MESH,
    )
    plain = [
        jnp.where(owns(at(way)), 0, 1) for d in range(places) for way in line_ways(d)
    ]
    met = sum(plain) + owners - jnp.where(is_owner, 1, 0)
    pl.semaphore_wait(barrier, jnp.where(lat > 0, met + 1, met))

    @pl.when(lat > 0)
    def _():
        edge_sum_copy.start()

    for way in line_ways(1):
        signal(met_sem.at[0], way)

    def to_device(src, dst, send_sem, recv_sem, device):
        return pltpu.make_async_remote_copy(
            src_ref=src,
            dst_ref=dst,
            send_sem=send_sem,
            recv_sem=recv_sem,
            device_id=(lat, device),
            device_id_type=MESH,
        )

    inner = FAN ** (places - 1)
    for shift in sorted(range(FAN), key=lambda i: -min(i, FAN - i)):
        for rest in itertools.product(range(reach // inner), range(FAN // CORES)):
            owner = rest[0] * inner + turned_digits[1][shift] + rest[1] * CORES + CORES - 1

            def start(owner=owner):
                mine_there = lines_in.at[lon]
                to_device(
                    lines.at[owner // CORES], mine_there, mean_send, line_recv, owner
                ).start()

            if shift:
                start()
            else:
                pl.when(owner != lon)(start)

    @pl.when(is_owner)
    def _():
        lines_in[pl.ds(lon, 1)] = lines[pl.ds(lon // CORES, 1)]

    for a in range(fields // SUB):
        edge[a * SUB : (a + 1) * SUB, :] = flat_warmth[pl.ds(a * SUB * pitch, SUB, stride=pitch), :]

    @pl.when(lat > 0)
    def _():
        edge_copy.start()

    width = 2 * times + 4

    def prepare(n):
        row = n * SUB
        here = pl.ds(row, SUB)
        split = splits[n % 2]
        lim = limit[here, :]
        for k in range(levels):
            wet = jnp.where(lim > k, 1.0, 0.0)
            v = [flow[t * levels + k, here, :] for t in range(times)]
            w = [
                0.5
                * (
                    warmth[t * levels + k, here, :]
                    + flat_warmth[pl.ds((t * levels + k) * pitch + row + 1, SUB), :]
                )
                for t in range(times)
            ]
            mean_v = functools.reduce(jnp.add, v) * (1.0 / times)
            mean_w = mean_warmth[k, here, :]
            cross = functools.reduce(
                jnp.add, [(v[t] - mean_v) * (w[t] - mean_w) for t in range(times)]
            ) * (1.0 / times)
            chunks = [x * wet for x in v] + [x * wet for x in w]
            chunks += [wet, mean_v * mean_w * wet, cross * wet, jnp.zeros_like(wet)]
            for c in range(0, width, 2):
                high, low = two_parts(jnp.concatenate(chunks[c : c + 2], axis=0))
                at_row = (k * width + c) * SUB
                split[at_row : at_row + 2 * SUB, 0:LANES] = high
                split[at_row : at_row + 2 * SUB, LANES : 2 * LANES] = low

    def contract(n):
        out = summed_over(splits[n % 2][...], hot_rows(n))
        for k in range(levels):
            count = piece(out, k * width + 2 * times, times)
            for half in range(2):
                acc = jnp.where(marks[times], count, 0.0)
                for t in range(times):
                    acc = jnp.where(marks[t], piece(out, k * width + half * times + t, t), acc)
                both = piece(out, k * width + 2 * times + 1 + half, times + 1)
                acc = jnp.where(marks[times + 1], both, acc)
                tiles[pl.ds(n * SUB * SUB + half * levels + k, SUB, stride=SUB), :] = straight(acc)

    def last_hot(size):
        iota = lax.broadcasted_iota(jnp.int32, (size, LANES), 0)
        tags = jnp.broadcast_to(label[last : last + 1, :], (size, LANES))
        hot = jnp.where(tags == iota, 1.0, 0.0).astype(jnp.bfloat16)
        return jnp.concatenate([hot, hot], axis=1)

    def edge_line_of_sums():
        lim = jnp.minimum(
            depth[last : last + 1, :], edge_sum_in[levels : levels + 1, :].astype(jnp.int32)
        )
        limit[last : last + 1, :] = lim
        wet = jnp.where(jnp.broadcast_to(lim, (SUB, LANES)) > sub % levels, 1.0, 0.0)
        here = flat_sums[pl.ds(last, levels, stride=pitch), :]
        mean = (here + edge_sum_in[0:levels, :]) * (0.5 / times)
        flat_mean[pl.ds(last, levels, stride=rows), :] = mean
        chunk = wet * jnp.concatenate([jnp.ones_like(mean), mean], axis=0)
        data = jnp.concatenate(two_parts(jnp.concatenate([chunk] * 2, axis=0)), axis=1)
        iota = lax.broadcasted_iota(jnp.int32, (LANES, LANES), 0)
        tags = jnp.broadcast_to(label[last : last + 1, :], (LANES, LANES))
        inside = (iota >= levels * BASINS) & (iota < 2 * levels * BASINS)
        hot = jnp.where(inside & (tags == iota % BASINS), 1.0, 0.0).astype(jnp.bfloat16)
        out = summed_over(data, jnp.concatenate([hot, hot], axis=1))[0:SUB, :]
        out = jnp.where(lane // BASINS - levels == sub % levels, out, 0.0)
        for shift in (1, 2):
            out = out + pltpu.roll(out, shift, axis=0)
        return jnp.concatenate([out[levels - 1 : levels, :], out[2 * levels - 1 :, :]], axis=0)

    def edge_tile():
        lim = limit[last : last + 1, :]
        wet = jnp.where(jnp.broadcast_to(lim, (SUB, LANES)) > sub % levels, 1.0, 0.0)
        x = []
        for t in range(times):
            v = flat_flow[pl.ds(t * levels * rows + last, levels, stride=rows), :]
            w = flat_warmth[pl.ds(t * levels * pitch + last, levels, stride=pitch), :]
            w = 0.5 * (w + edge_in[t * levels : (t + 1) * levels, :])
            x.append(jnp.concatenate([v, w], axis=0))
        mean = functools.reduce(jnp.add, x) * (1.0 / times)
        devs = [y - mean for y in x]
        cross = functools.reduce(jnp.add, [y * other_half(y) for y in devs]) * (1.0 / times)
        both = jnp.where(sub < levels, mean * other_half(mean), cross)
        chunks = jnp.concatenate([y * wet for y in x] + [wet, both * wet], axis=0)
        data = jnp.concatenate(two_parts(chunks), axis=1)
        out = summed_over(data, last_hot(LANES))
        return functools.reduce(jnp.add, [piece(out, m, m) for m in range(slots)])

    def other_half(x):
        return pltpu.roll(x, levels, axis=0)

    def wait_for(ref, count, send_sem, recv_sem):
        part = pl.ds(0, count)
        return pltpu.make_async_remote_copy(
            src_ref=ref.at[part],
            dst_ref=ref.at[part],
            send_sem=send_sem,
            recv_sem=recv_sem,
            device_id=(lat, lon),
            device_id_type=MESH,
        )

    cuts = (0, steps // 2, steps)
    for low_cut, high_cut in itertools.pairwise(cuts):
        wait_rows(flow_hbm, flow, low_cut, high_cut, flow_sem.at[2 * low_cut // steps])
        for n in range(low_cut, high_cut):
            prepare(n)
            if n:
                contract(n - 1)
        if high_cut < steps:
            pl.semaphore_wait(met_sem.at[0], FAN - 1)
            for way in line_ways(places - 1):
                signal(met_sem.at[1], way)
    contract(steps - 1)
    core = lax.rem(lon, CORES)
    partner = lon + 1 - CORES * core

    def tile(ref, row):
        return ref.at[pl.ds(pl.multiple_of(row * SUB, SUB), SUB)]

    pairs = rows // CORES
    for i in range(pairs):
        to_device(
            tile(tiles, CORES * i + 1 - core), tile(tiles_near, i), sum_send, near_recv, partner
        ).start()

    every_line = wait_for(lines_in, lons - 1, mean_send, line_recv)
    every_bar = wait_for(bar_in, owners, mean_send, bar_recv)
    fewer_bars = wait_for(bar_in, owners - 1, mean_send, bar_recv)
    every_edge_line = wait_for(edge_lines, lons - 1, edge_line_send, edge_line_recv)
    every_near = wait_for(tiles_near, pairs * SUB, sum_send, near_recv)
    every_tile = wait_for(tiles_in, (pairs - 1) * SUB, sum_send, tile_recv)
    every_last = wait_for(tiles_last, (lons - 1) * SUB, sum_send, tile_recv)

    def tree_sum(parts):
        while len(parts) > 1:
            parts = [sum(parts[i : i + 2][1:], parts[i]) for i in range(0, len(parts), 2)]
        return parts[0]

    def ratio(total):
        return total / jnp.maximum(pltpu.roll(total, levels * BASINS, axis=1), 1.0)

    pl.semaphore_wait(met_sem.at[1], FAN - 1)

    every_near.wait_recv()
    for i in range(pairs):
        own = pl.ds(pl.multiple_of((CORES * i + core) * SUB, SUB), SUB)
        tiles[own, :] = tiles[own, :] + tiles_near[i * SUB : (i + 1) * SUB, :]
    for way in far_first():
        if way[0] % CORES == 0:
            peer = at(way)

            @pl.when(peer != last)
            def _():
                to_device(
                    tile(tiles, peer), tile(tiles_in, lon // CORES), sum_send, tile_recv, peer
                ).start()

    @pl.when(lat < lats - 1)
    def _():
        edge_sum_copy.wait_recv()

    @pl.when(lat == lats - 1)
    def _():
        edge_sum_in[...] = jnp.zeros_like(edge_sum_in)

    line = edge_line_of_sums()
    edge_line[...] = line
    edge_lines[pl.ds(lon, 1)] = line[None]
    for peer in map(at, far_first()):
        to_device(edge_line, edge_lines.at[lon], edge_line_send, edge_line_recv, peer).start()

    @pl.when(is_owner)
    def _():
        every_line.wait_recv()
        bar[...] = ratio(tree_sum([lines_in[p] for p in range(lons)]))
        bar_in[pl.ds(lon // CORES, 1)] = bar[...][None]
        for peer in map(at, far_first()):
            to_device(bar, bar_in.at[lon // CORES], mean_send, bar_recv, peer).start()

    @pl.when(lat < lats - 1)
    def _():
        edge_copy.wait_recv()

    @pl.when(lat == lats - 1)
    def _():
        edge_in[...] = jnp.zeros_like(edge_in)

    last_tile[...] = edge_tile()
    tiles_last[mine, :] = last_tile[...]

    @pl.when(lon != last)
    def _():
        to_device(last_tile, tile(tiles_last, lon), sum_send, tile_recv, last).start()

    def tiles_of(ref, count):
        return [ref[SUB * p : SUB * (p + 1), :] for p in range(count)]

    @pl.when(lon != last)
    def _():
        every_tile.wait_recv()
        own_total[...] = tree_sum([tiles[mine, :], *tiles_of(tiles_in, pairs)])

    @pl.when(lon == last)
    def _():
        every_last.wait_recv()
        own_total[...] = tree_sum(tiles_of(tiles_last, lons))

    total = own_total[...]

    def moved(x, lanes):
        return pltpu.roll(x, (-lanes) % LANES, axis=1)

    count = moved(total, BASINS * times)
    first = lane < BASINS
    divisor = jnp.maximum(count, 1.0)
    time_sums = total
    for t in range(1, times):
        time_sums = time_sums + moved(total, BASINS * t)
    bars = jnp.where(first, time_sums / divisor * (1.0 / times), 0.0)

    bars_w = other_half(bars)
    flow_part = scaling * count * bars * bars_w
    swing = jnp.zeros_like(total)
    for t in range(times):
        dev = (moved(total, 10 * t) if t else total) / divisor - bars
        swing = swing + dev * other_half(dev)
    swing = scaling * count * (swing * (1.0 / times))
    both = moved(total, 10 * (times + 1))
    steady = scaling * both - flow_part
    transient = scaling * other_half(both) - swing
    for q, value in enumerate((flow_part, steady, swing, transient)):
        for k in range(levels):
            transport_ref[q, k] = value[k : k + 1, 0:BASINS]

    every_edge_line.wait_recv()
    total = tree_sum([edge_lines[p] for p in range(lons)])
    last_bars = total[1:2, :] / jnp.maximum(total[0:1, :], 1.0)
    @pl.when(is_owner)
    def _():
        fewer_bars.wait_recv()

    @pl.when(jnp.logical_not(is_owner))
    def _():
        every_bar.wait_recv()

    for n in range(steps):
        here = slice(n * SUB, (n + 1) * SUB)
        table = bar_in[n * SUB // share : (n + 1) * SUB // share].reshape(SUB, LANES)
        if n == steps - 1:
            table = jnp.where(sub == SUB - 1, jnp.broadcast_to(last_bars, table.shape), table)
        lim = limit[here, :]
        tags = label[here, :]
        for k in range(levels):
            cell = jnp.take_along_axis(
                table, tags + (levels + k) * BASINS, axis=1, mode="promise_in_bounds"
            )
            eddy_ref[k, here, :] = jnp.where(lim > k, mean_warmth[k, here, :] - cell, 0.0)

    every_edge_line.wait_send()

    def wait_sent(count, semaphore):
        wait_for(flat_flow, count, semaphore, edge_recv).wait_send()

    @pl.when(core == CORES - 1)
    def _():
        wait_sent((2 * pairs - 1) * SUB, sum_send)

    @pl.when(core < CORES - 1)
    def _():
        wait_sent(2 * pairs * SUB, sum_send)

    @pl.when(is_owner)
    def _():
        wait_sent((owners - 1 + lons - 1) * share, mean_send)

    @pl.when(jnp.logical_not(is_owner))
    def _():
        wait_sent(owners * share, mean_send)

    @pl.when(lat > 0)
    def _():
        wait_sent(fields + 2 * levels, edge_send)


def write_out(eddy, transport, eddy_out, transport_out, sem):
    copies = [
        pltpu.make_async_copy(eddy, eddy_out, sem.at[0]),
        pltpu.make_async_copy(transport, transport_out, sem.at[1]),
    ]
    for copy in copies:
        copy.start()
    for copy in copies:
        copy.wait()


def shards(lats, lons, flow, warmth, flag, floor, label):
    times, levels, rows, cols = flow.shape
    fields = times * levels
    pitch = rows + SUB
    scaling = 1.0 / math.sqrt(cols * lons)
    owners = lons // OWNER_PART
    share = rows // owners
    dims = (times, levels, rows, pitch, lats, lons, owners, share, scaling)
    local = pl.BlockSpec(memory_space=pltpu.VMEM)
    dma = pltpu.SemaphoreType.DMA
    f32 = jnp.float32
    eddy, transport = pl.pallas_call(
        functools.partial(kernel, dims),
        out_shape=(
            pltpu.VMEM((levels, rows, cols), f32),
            pltpu.VMEM((4, levels, 1, BASINS), f32),
        ),
        in_specs=[pl.BlockSpec(memory_space=pltpu.HBM)] * 5,
        out_specs=(local, local),
        scratch_shapes=[
            pltpu.VMEM((fields, rows, cols), f32),
            pltpu.VMEM((fields, pitch, cols), f32),
            pltpu.VMEM((rows, cols), jnp.int32),
            pltpu.VMEM((rows, cols), jnp.int32),
            pltpu.VMEM((rows, cols), jnp.int32),
            pltpu.VMEM((pitch, cols), jnp.int32),
            pltpu.VMEM((rows, cols), jnp.int32),
            pltpu.VMEM((levels, rows, cols), f32),
            pltpu.VMEM((levels, pitch, cols), f32),
            pltpu.VMEM((levels * (2 * times + 4) * SUB, 2 * cols), jnp.bfloat16),
            pltpu.VMEM((levels * (2 * times + 4) * SUB, 2 * cols), jnp.bfloat16),
            pltpu.VMEM((fields, cols), f32),
            pltpu.VMEM((fields, cols), f32),
            pltpu.VMEM((2 * levels, cols), f32),
            pltpu.VMEM((2 * levels, cols), f32),
            pltpu.VMEM((rows * SUB, cols), f32),
            pltpu.VMEM((rows // CORES * SUB, cols), f32),
            pltpu.VMEM((share, cols), f32),
            pltpu.VMEM((owners, share, cols), f32),
            pltpu.VMEM((2, cols), f32),
            pltpu.VMEM((lons, 2, cols), f32),
            pltpu.VMEM((owners, share, cols), f32),
            pltpu.VMEM((lons, share, cols), f32),
            pltpu.VMEM((rows // CORES * SUB, cols), f32),
            pltpu.VMEM((rows * SUB, cols), f32),
            pltpu.VMEM((SUB, cols), f32),
            pltpu.VMEM((SUB, cols), f32),
            dma((2,)),
            dma((3,)),
            dma,
        ]
        + [dma] * 11
        + [
            pltpu.SemaphoreType.REGULAR((2,)),
        ],
        compiler_params=pltpu.CompilerParams(
            collective_id=0, has_side_effects=True, vmem_limit_bytes=66879488
        ),
    )(
        flow.reshape(fields, rows, cols),
        warmth.reshape(fields, rows, cols),
        flag,
        floor,
        label,
    )
    eddy, transport = pl.pallas_call(
        write_out,
        out_shape=tuple(jax.ShapeDtypeStruct(a.shape, a.dtype) for a in (eddy, transport)),
        in_specs=[local] * 2,
        out_specs=[pl.BlockSpec(memory_space=pltpu.HBM)] * 2,
        scratch_shapes=[dma((2,))],
        compiler_params=pltpu.CompilerParams(vmem_limit_bytes=2**20),
    )(eddy, transport)
    return eddy, jnp.transpose(transport, (0, 3, 1, 2))


def solution(mesh):
    return jax.shard_map(
        functools.partial(shards, mesh.shape["lat"], mesh.shape["lon"]),
        mesh=mesh,
        in_specs=(
            P(None, None, "lat", "lon"),
            P(None, None, "lat", "lon"),
            P("lat", "lon"),
            P("lat", "lon"),
            P("lat", "lon"),
        ),
        out_specs=(P(None, "lat", "lon"), P(None, None, None, ("lat", "lon"))),
        check_vma=False,
    )
```

```python
import functools
import itertools
import math

import jax
import jax.numpy as jnp
from jax import lax
from jax.experimental import pallas as pl
from jax.experimental.pallas import tpu as pltpu
from jax.sharding import PartitionSpec as P

BASINS = 10
OWNER_PART = 8
CORES = 2
FAN = 4
GROUP = 16
SUB = 8
LANES = 128
MESH = pl.DeviceIdType.MESH


def kernel(
    dims,
    flow_hbm,
    warmth_hbm,
    flag_hbm,
    floor_hbm,
    label_hbm,
    eddy_ref,
    transport_ref,
    flow,
    warmth,
    flag,
    floor,
    label,
    depth,
    limit,
    mean_warmth,
    sums,
    split_even,
    split_odd,
    edge,
    edge_in,
    edge_sum,
    edge_sum_in,
    tiles,
    tiles_in,
    bar,
    bar_in,
    edge_line,
    edge_lines,
    lines,
    lines_in,
    tiles_near,
    tiles_last,
    last_tile,
    own_total,
    flow_sem,
    warmth_sem,
    small_sem,
    edge_send,
    edge_recv,
    edge_sum_recv,
    near_recv,
    tile_recv,
    bar_recv,
    line_recv,
    edge_line_send,
    edge_line_recv,
    sum_send,
    mean_send,
    met_sem,
):
    splits = (split_even, split_odd)
    times, levels, rows, pitch, lats, lons, owners, share, scaling = dims
    steps = rows // SUB
    lat, lon = lax.axis_index("lat"), lax.axis_index("lon")
    fields = times * levels
    last = rows - 1
    mine = pl.ds(pl.multiple_of(lon * SUB, SUB), SUB)
    places = round(math.log(lons, FAN))
    flat_flow = flow.reshape(fields * rows, LANES)
    flat_sums = sums.reshape(levels * pitch, LANES)
    flat_mean = mean_warmth.reshape(levels * rows, LANES)
    flat_warmth = warmth.reshape(fields * pitch, LANES)

    def flow_copy(n):
        part = pl.ds(pl.multiple_of(n * SUB, SUB), SUB)
        return pltpu.make_async_copy(flow_hbm.at[:, part], flow.at[:, part], flow_sem.at[2 * n // steps])

    def warmth_copy(n):
        part = pl.ds(pl.multiple_of(n * SUB, SUB), SUB)
        return pltpu.make_async_copy(warmth_hbm.at[:, part], warmth.at[:, part], warmth_sem.at[min(n, 1) + 2 * n // steps])

    smalls = [
        pltpu.make_async_copy(flag_hbm, flag, small_sem),
        pltpu.make_async_copy(floor_hbm, floor, small_sem),
        pltpu.make_async_copy(label_hbm, label, small_sem),
    ]

    def wait_rows(source, target, first, end, sem):
        part = pl.ds(first * SUB, (end - first) * SUB)
        pltpu.make_async_copy(source.at[:, part], target.at[:, part], sem).wait()

    warmth_copy(0).start()
    for copy in smalls:
        copy.start()

    barrier = pltpu.get_barrier_semaphore()
    turned_digits = [
        [lax.rem(lon // FAN**d + i, FAN) * FAN**d for i in range(FAN)] for d in range(places)
    ]
    reach = owners * CORES

    def owns(device):
        return (device < reach) & (lax.rem(device, CORES) == CORES - 1)

    is_owner = owns(lon)

    def far_first():
        ways = itertools.product(range(FAN), repeat=places)
        hops = lambda way: sum(min(i, FAN - i) for i in way[1:]) + (way[0] > 0)
        return [way for way in sorted(ways, key=hops, reverse=True) if any(way)]

    def at(way):
        return sum(turned_digits[d][way[d]] for d in range(places))

    def signal(semaphore, way):
        pl.semaphore_signal(semaphore, inc=1, device_id=(lat, at(way)), device_id_type=MESH)

    def line_ways(d):
        return [way for way in far_first() if way[d] and sum(i > 0 for i in way) == 1]

    @pl.when(is_owner)
    def _():
        for way in far_first():
            signal(barrier, way)

    @pl.when(jnp.logical_not(is_owner))
    def _():
        for way in far_first():
            if sum(i > 0 for i in way) == 1:
                signal(barrier, way)

    @pl.when(lat < lats - 1)
    def _():
        pl.semaphore_signal(barrier, inc=1, device_id=(lat + 1, lon), device_id_type=MESH)

    for n in range(1, steps):
        warmth_copy(n).start()
    for a in range(fields // SUB):
        flat_warmth[pl.ds(a * SUB * pitch + rows, SUB, stride=pitch), :] = jnp.zeros(
            (SUB, LANES), jnp.float32
        )
    for k in range(levels):
        flat_sums[k * pitch + rows : k * pitch + rows + SUB, :] = jnp.zeros(
            (SUB, LANES), jnp.float32
        )
    depth[rows : rows + SUB, :] = jnp.zeros((SUB, LANES), jnp.int32)
    own_chip = pl.ds(pl.multiple_of(lon // CORES * SUB, SUB), SUB)
    tiles_in[own_chip, :] = jnp.zeros((SUB, LANES), jnp.float32)
    pltpu.make_async_copy(
        flow_hbm.at[0 : len(smalls)], flow.at[0 : len(smalls)], small_sem
    ).wait()
    warmth_copy(0).wait()
    for n in range(steps):
        flow_copy(n).start()
    depth[0:rows, :] = flag[...] * floor[...]
    lane = lax.broadcasted_iota(jnp.int32, (SUB, LANES), 1)
    sub = lax.broadcasted_iota(jnp.int32, (SUB, LANES), 0)
    slots = times + 2
    turned = (lane + GROUP * sub) % LANES
    marks = [(turned >= BASINS * m) & (turned < BASINS * (m + 1)) for m in range(slots)]

    def two_parts(x):
        high = x.astype(jnp.bfloat16)
        return high, (x - high.astype(jnp.float32)).astype(jnp.bfloat16)

    def in_three(x):
        high = x.astype(jnp.bfloat16).astype(jnp.float32)
        rest = x - high
        middle = rest.astype(jnp.bfloat16).astype(jnp.float32)
        return [high, middle, rest - middle]

    def folded(out, size):
        return out[0:size, :] + out[size : 2 * size, :] + out[2 * size : 3 * size, :]

    def straight(x):
        return pltpu.roll(x, 0, axis=1, stride=GROUP, stride_axis=0)

    def hot_rows(n):
        iota = lax.broadcasted_iota(jnp.int32, (GROUP, LANES), 0)
        tags = label[n * SUB : (n + 1) * SUB, :]
        hot = jnp.concatenate(
            [
                jnp.where(
                    jnp.broadcast_to(tags[r : r + 1, :], (GROUP, LANES)) == iota, 1.0, 0.0
                )
                for r in (0, *range(SUB - 1, 0, -1))
            ],
            axis=0,
        ).astype(jnp.bfloat16)
        return jnp.concatenate([hot, hot], axis=1)

    def summed_over(data, hot):
        return lax.dot_general(
            data, hot, (((1,), (1,)), ((), ())), preferred_element_type=jnp.float32
        )

    def piece(out, c, m):
        x = out[c * SUB : (c + 1) * SUB, :]
        return pltpu.roll(x, BASINS * m, axis=1) if m else x

    def sum_times(n):
        here = pl.ds(n * SUB, SUB)
        for k in range(levels):
            sums[k, here, :] = functools.reduce(
                jnp.add, [warmth[t * levels + k, here, :] for t in range(times)]
            )

    wait_rows(warmth_hbm, warmth, 1, steps // 2, warmth_sem.at[1])
    for n in range(steps // 2):
        sum_times(n)
    wait_rows(warmth_hbm, warmth, steps // 2, steps, warmth_sem.at[2])
    for n in range(steps // 2, steps):
        sum_times(n)
    for n in range(steps):
        here = pl.ds(n * SUB, SUB)
        lim = jnp.minimum(depth[here, :], depth[pl.ds(n * SUB + 1, SUB), :])
        limit[here, :] = lim
        chunks = []
        for k in range(levels):
            wet = jnp.where(lim > k, 1.0, 0.0)
            mean_w = (sums[k, here, :] + flat_sums[pl.ds(k * pitch + n * SUB + 1, SUB), :]) * (
                0.5 / times
            )
            mean_warmth[k, here, :] = mean_w
            chunks += [wet, mean_w * wet]
        data = jnp.concatenate(in_three(jnp.concatenate(chunks, axis=0)), axis=0)
        out = summed_over(data.astype(jnp.bfloat16), hot_rows(n)[:, 0:LANES])
        out = folded(out, 2 * levels * SUB)
        line = jnp.zeros((SUB, LANES), jnp.float32)
        for k in range(levels):
            line = jnp.where(marks[k], piece(out, 2 * k, k), line)
            line = jnp.where(marks[levels + k], piece(out, 2 * k + 1, levels + k), line)
        line = straight(line)
        lines[n * SUB // share : (n + 1) * SUB // share] = line.reshape(
            SUB // share, share, LANES
        )

    edge_sum[...] = jnp.concatenate(
        [flat_sums[pl.ds(0, levels, stride=pitch), :], depth[0:levels, :].astype(jnp.float32)],
        axis=0,
    )
    edge_sum_copy = pltpu.make_async_remote_copy(
        src_ref=edge_sum,
        dst_ref=edge_sum_in,
        send_sem=edge_send,
        recv_sem=edge_sum_recv,
        device_id=(lat - 1, lon),
        device_id_type=MESH,
    )
    edge_copy = pltpu.make_async_remote_copy(
        src_ref=edge,
        dst_ref=edge_in,
        send_sem=edge_send,
        recv_sem=edge_recv,
        device_id=(lat - 1, lon),
        device_id_type=MESH,
    )
    plain = [
        jnp.where(owns(at(way)), 0, 1) for d in range(places) for way in line_ways(d)
    ]
    met = sum(plain) + owners - jnp.where(is_owner, 1, 0)
    pl.semaphore_wait(barrier, jnp.where(lat > 0, met + 1, met))

    @pl.when(lat > 0)
    def _():
        edge_sum_copy.start()

    for way in line_ways(1):
        signal(met_sem.at[0], way)

    def to_device(src, dst, send_sem, recv_sem, device):
        return pltpu.make_async_remote_copy(
            src_ref=src,
            dst_ref=dst,
            send_sem=send_sem,
            recv_sem=recv_sem,
            device_id=(lat, device),
            device_id_type=MESH,
        )

    inner = FAN ** (places - 1)
    for shift in sorted(range(FAN), key=lambda i: -min(i, FAN - i)):
        for rest in itertools.product(range(reach // inner), range(FAN // CORES)):
            owner = rest[0] * inner + turned_digits[1][shift] + rest[1] * CORES + CORES - 1

            def start(owner=owner):
                mine_there = lines_in.at[lon]
                to_device(
                    lines.at[owner // CORES], mine_there, mean_send, line_recv, owner
                ).start()

            if shift:
                start()
            else:
                pl.when(owner != lon)(start)

    @pl.when(is_owner)
    def _():
        lines_in[pl.ds(lon, 1)] = lines[pl.ds(lon // CORES, 1)]

    for a in range(fields // SUB):
        edge[a * SUB : (a + 1) * SUB, :] = flat_warmth[pl.ds(a * SUB * pitch, SUB, stride=pitch), :]

    @pl.when(lat > 0)
    def _():
        edge_copy.start()

    width = 2 * times + 4

    def prepare(n):
        row = n * SUB
        here = pl.ds(row, SUB)
        split = splits[n % 2]
        lim = limit[here, :]
        for k in range(levels):
            wet = jnp.where(lim > k, 1.0, 0.0)
            v = [flow[t * levels + k, here, :] for t in range(times)]
            w = [
                0.5
                * (
                    warmth[t * levels + k, here, :]
                    + flat_warmth[pl.ds((t * levels + k) * pitch + row + 1, SUB), :]
                )
                for t in range(times)
            ]
            mean_v = functools.reduce(jnp.add, v) * (1.0 / times)
            mean_w = mean_warmth[k, here, :]
            cross = functools.reduce(
                jnp.add, [(v[t] - mean_v) * (w[t] - mean_w) for t in range(times)]
            ) * (1.0 / times)
            chunks = [x * wet for x in v] + [x * wet for x in w]
            chunks += [wet, mean_v * mean_w * wet, cross * wet, jnp.zeros_like(wet)]
            for c in range(0, width, 2):
                high, low = two_parts(jnp.concatenate(chunks[c : c + 2], axis=0))
                at_row = (k * width + c) * SUB
                split[at_row : at_row + 2 * SUB, 0:LANES] = high
                split[at_row : at_row + 2 * SUB, LANES : 2 * LANES] = low

    def contract(n):
        out = summed_over(splits[n % 2][...], hot_rows(n))
        for k in range(levels):
            count = piece(out, k * width + 2 * times, times)
            for half in range(2):
                acc = jnp.where(marks[times], count, 0.0)
                for t in range(times):
                    acc = jnp.where(marks[t], piece(out, k * width + half * times + t, t), acc)
                both = piece(out, k * width + 2 * times + 1 + half, times + 1)
                acc = jnp.where(marks[times + 1], both, acc)
                tiles[pl.ds(n * SUB * SUB + half * levels + k, SUB, stride=SUB), :] = straight(acc)

    def last_hot(size):
        iota = lax.broadcasted_iota(jnp.int32, (size, LANES), 0)
        tags = jnp.broadcast_to(label[last : last + 1, :], (size, LANES))
        hot = jnp.where(tags == iota, 1.0, 0.0).astype(jnp.bfloat16)
        return jnp.concatenate([hot, hot], axis=1)

    def edge_line_of_sums():
        lim = jnp.minimum(
            depth[last : last + 1, :], edge_sum_in[levels : levels + 1, :].astype(jnp.int32)
        )
        limit[last : last + 1, :] = lim
        wet = jnp.where(jnp.broadcast_to(lim, (SUB, LANES)) > sub % levels, 1.0, 0.0)
        here = flat_sums[pl.ds(last, levels, stride=pitch), :]
        mean = (here + edge_sum_in[0:levels, :]) * (0.5 / times)
        flat_mean[pl.ds(last, levels, stride=rows), :] = mean
        chunk = wet * jnp.concatenate([jnp.ones_like(mean), mean], axis=0)
        data = jnp.concatenate([*in_three(chunk), jnp.zeros_like(chunk)], axis=0)
        iota = lax.broadcasted_iota(jnp.int32, (LANES, LANES), 0)
        tags = jnp.broadcast_to(label[last : last + 1, :], (LANES, LANES))
        inside = (iota >= levels * BASINS) & (iota < 2 * levels * BASINS)
        hot = jnp.where(inside & (tags == iota % BASINS), 1.0, 0.0).astype(jnp.bfloat16)
        out = folded(summed_over(data.astype(jnp.bfloat16), hot), SUB)
        out = jnp.where(lane // BASINS - levels == sub % levels, out, 0.0)
        for shift in (1, 2):
            out = out + pltpu.roll(out, shift, axis=0)
        return jnp.concatenate([out[levels - 1 : levels, :], out[2 * levels - 1 :, :]], axis=0)

    def edge_tile():
        lim = limit[last : last + 1, :]
        wet = jnp.where(jnp.broadcast_to(lim, (SUB, LANES)) > sub % levels, 1.0, 0.0)
        x = []
        for t in range(times):
            v = flat_flow[pl.ds(t * levels * rows + last, levels, stride=rows), :]
            w = flat_warmth[pl.ds(t * levels * pitch + last, levels, stride=pitch), :]
            w = 0.5 * (w + edge_in[t * levels : (t + 1) * levels, :])
            x.append(jnp.concatenate([v, w], axis=0))
        mean = functools.reduce(jnp.add, x) * (1.0 / times)
        devs = [y - mean for y in x]
        cross = functools.reduce(jnp.add, [y * other_half(y) for y in devs]) * (1.0 / times)
        both = jnp.where(sub < levels, mean * other_half(mean), cross)
        chunks = jnp.concatenate([y * wet for y in x] + [wet, both * wet], axis=0)
        data = jnp.concatenate(two_parts(chunks), axis=1)
        out = summed_over(data, last_hot(LANES))
        return functools.reduce(jnp.add, [piece(out, m, m) for m in range(slots)])

    def other_half(x):
        return pltpu.roll(x, levels, axis=0)

    def wait_for(ref, count, send_sem, recv_sem):
        part = pl.ds(0, count)
        return pltpu.make_async_remote_copy(
            src_ref=ref.at[part],
            dst_ref=ref.at[part],
            send_sem=send_sem,
            recv_sem=recv_sem,
            device_id=(lat, lon),
            device_id_type=MESH,
        )

    cuts = (0, steps // 2, steps)
    for low_cut, high_cut in itertools.pairwise(cuts):
        wait_rows(flow_hbm, flow, low_cut, high_cut, flow_sem.at[2 * low_cut // steps])
        for n in range(low_cut, high_cut):
            prepare(n)
            if n:
                contract(n - 1)
        if high_cut < steps:
            pl.semaphore_wait(met_sem.at[0], FAN - 1)
            for way in line_ways(places - 1):
                signal(met_sem.at[1], way)
    contract(steps - 1)
    core = lax.rem(lon, CORES)
    partner = lon + 1 - CORES * core

    def tile(ref, row):
        return ref.at[pl.ds(pl.multiple_of(row * SUB, SUB), SUB)]

    pairs = rows // CORES
    for i in range(pairs):
        to_device(
            tile(tiles, CORES * i + 1 - core), tile(tiles_near, i), sum_send, near_recv, partner
        ).start()

    every_line = wait_for(lines_in, lons - 1, mean_send, line_recv)
    every_bar = wait_for(bar_in, owners, mean_send, bar_recv)
    fewer_bars = wait_for(bar_in, owners - 1, mean_send, bar_recv)
    every_edge_line = wait_for(edge_lines, lons - 1, edge_line_send, edge_line_recv)
    every_near = wait_for(tiles_near, pairs * SUB, sum_send, near_recv)
    every_tile = wait_for(tiles_in, (pairs - 1) * SUB, sum_send, tile_recv)
    every_last = wait_for(tiles_last, (lons - 1) * SUB, sum_send, tile_recv)

    def tree_sum(parts):
        while len(parts) > 1:
            parts = [sum(parts[i : i + 2][1:], parts[i]) for i in range(0, len(parts), 2)]
        return parts[0]

    def ratio(total):
        return total / jnp.maximum(pltpu.roll(total, levels * BASINS, axis=1), 1.0)

    pl.semaphore_wait(met_sem.at[1], FAN - 1)

    every_near.wait_recv()
    for i in range(pairs):
        own = pl.ds(pl.multiple_of((CORES * i + core) * SUB, SUB), SUB)
        tiles[own, :] = tiles[own, :] + tiles_near[i * SUB : (i + 1) * SUB, :]
    for way in far_first():
        if way[0] % CORES == 0:
            peer = at(way)

            @pl.when(peer != last)
            def _():
                to_device(
                    tile(tiles, peer), tile(tiles_in, lon // CORES), sum_send, tile_recv, peer
                ).start()

    @pl.when(lat < lats - 1)
    def _():
        edge_sum_copy.wait_recv()

    @pl.when(lat == lats - 1)
    def _():
        edge_sum_in[...] = jnp.zeros_like(edge_sum_in)

    line = edge_line_of_sums()
    edge_line[...] = line
    edge_lines[pl.ds(lon, 1)] = line[None]
    for peer in map(at, far_first()):
        to_device(edge_line, edge_lines.at[lon], edge_line_send, edge_line_recv, peer).start()

    @pl.when(is_owner)
    def _():
        every_line.wait_recv()
        bar[...] = ratio(tree_sum([lines_in[p] for p in range(lons)]))
        bar_in[pl.ds(lon // CORES, 1)] = bar[...][None]
        for peer in map(at, far_first()):
            to_device(bar, bar_in.at[lon // CORES], mean_send, bar_recv, peer).start()

    @pl.when(lat < lats - 1)
    def _():
        edge_copy.wait_recv()

    @pl.when(lat == lats - 1)
    def _():
        edge_in[...] = jnp.zeros_like(edge_in)

    last_tile[...] = edge_tile()
    tiles_last[mine, :] = last_tile[...]

    @pl.when(lon != last)
    def _():
        to_device(last_tile, tile(tiles_last, lon), sum_send, tile_recv, last).start()

    def tiles_of(ref, count):
        return [ref[SUB * p : SUB * (p + 1), :] for p in range(count)]

    @pl.when(lon != last)
    def _():
        every_tile.wait_recv()
        own_total[...] = tree_sum([tiles[mine, :], *tiles_of(tiles_in, pairs)])

    @pl.when(lon == last)
    def _():
        every_last.wait_recv()
        own_total[...] = tree_sum(tiles_of(tiles_last, lons))

    total = own_total[...]

    def moved(x, lanes):
        return pltpu.roll(x, (-lanes) % LANES, axis=1)

    count = moved(total, BASINS * times)
    first = lane < BASINS
    divisor = jnp.maximum(count, 1.0)
    time_sums = total
    for t in range(1, times):
        time_sums = time_sums + moved(total, BASINS * t)
    bars = jnp.where(first, time_sums / divisor * (1.0 / times), 0.0)

    bars_w = other_half(bars)
    flow_part = scaling * count * bars * bars_w
    swing = jnp.zeros_like(total)
    for t in range(times):
        dev = (moved(total, 10 * t) if t else total) / divisor - bars
        swing = swing + dev * other_half(dev)
    swing = scaling * count * (swing * (1.0 / times))
    both = moved(total, 10 * (times + 1))
    steady = scaling * both - flow_part
    transient = scaling * other_half(both) - swing
    for q, value in enumerate((flow_part, steady, swing, transient)):
        for k in range(levels):
            transport_ref[q, k] = value[k : k + 1, 0:BASINS]

    every_edge_line.wait_recv()
    total = tree_sum([edge_lines[p] for p in range(lons)])
    last_bars = total[1:2, :] / jnp.maximum(total[0:1, :], 1.0)
    @pl.when(is_owner)
    def _():
        fewer_bars.wait_recv()

    @pl.when(jnp.logical_not(is_owner))
    def _():
        every_bar.wait_recv()

    for n in range(steps):
        here = slice(n * SUB, (n + 1) * SUB)
        table = bar_in[n * SUB // share : (n + 1) * SUB // share].reshape(SUB, LANES)
        if n == steps - 1:
            table = jnp.where(sub == SUB - 1, jnp.broadcast_to(last_bars, table.shape), table)
        lim = limit[here, :]
        tags = label[here, :]
        for k in range(levels):
            cell = jnp.take_along_axis(
                table, tags + (levels + k) * BASINS, axis=1, mode="promise_in_bounds"
            )
            eddy_ref[k, here, :] = jnp.where(lim > k, mean_warmth[k, here, :] - cell, 0.0)

    every_edge_line.wait_send()

    def wait_sent(count, semaphore):
        wait_for(flat_flow, count, semaphore, edge_recv).wait_send()

    @pl.when(core == CORES - 1)
    def _():
        wait_sent((2 * pairs - 1) * SUB, sum_send)

    @pl.when(core < CORES - 1)
    def _():
        wait_sent(2 * pairs * SUB, sum_send)

    @pl.when(is_owner)
    def _():
        wait_sent((owners - 1 + lons - 1) * share, mean_send)

    @pl.when(jnp.logical_not(is_owner))
    def _():
        wait_sent(owners * share, mean_send)

    @pl.when(lat > 0)
    def _():
        wait_sent(fields + 2 * levels, edge_send)


def write_out(eddy, transport, eddy_out, transport_out, sem):
    copies = [
        pltpu.make_async_copy(eddy, eddy_out, sem.at[0]),
        pltpu.make_async_copy(transport, transport_out, sem.at[1]),
    ]
    for copy in copies:
        copy.start()
    for copy in copies:
        copy.wait()


def shards(lats, lons, flow, warmth, flag, floor, label):
    times, levels, rows, cols = flow.shape
    fields = times * levels
    pitch = rows + SUB
    scaling = 1.0 / math.sqrt(cols * lons)
    owners = lons // OWNER_PART
    share = rows // owners
    dims = (times, levels, rows, pitch, lats, lons, owners, share, scaling)
    local = pl.BlockSpec(memory_space=pltpu.VMEM)
    dma = pltpu.SemaphoreType.DMA
    f32 = jnp.float32
    eddy, transport = pl.pallas_call(
        functools.partial(kernel, dims),
        out_shape=(
            pltpu.VMEM((levels, rows, cols), f32),
            pltpu.VMEM((4, levels, 1, BASINS), f32),
        ),
        in_specs=[pl.BlockSpec(memory_space=pltpu.HBM)] * 5,
        out_specs=(local, local),
        scratch_shapes=[
            pltpu.VMEM((fields, rows, cols), f32),
            pltpu.VMEM((fields, pitch, cols), f32),
            pltpu.VMEM((rows, cols), jnp.int32),
            pltpu.VMEM((rows, cols), jnp.int32),
            pltpu.VMEM((rows, cols), jnp.int32),
            pltpu.VMEM((pitch, cols), jnp.int32),
            pltpu.VMEM((rows, cols), jnp.int32),
            pltpu.VMEM((levels, rows, cols), f32),
            pltpu.VMEM((levels, pitch, cols), f32),
            pltpu.VMEM((levels * (2 * times + 4) * SUB, 2 * cols), jnp.bfloat16),
            pltpu.VMEM((levels * (2 * times + 4) * SUB, 2 * cols), jnp.bfloat16),
            pltpu.VMEM((fields, cols), f32),
            pltpu.VMEM((fields, cols), f32),
            pltpu.VMEM((2 * levels, cols), f32),
            pltpu.VMEM((2 * levels, cols), f32),
            pltpu.VMEM((rows * SUB, cols), f32),
            pltpu.VMEM((rows // CORES * SUB, cols), f32),
            pltpu.VMEM((share, cols), f32),
            pltpu.VMEM((owners, share, cols), f32),
            pltpu.VMEM((2, cols), f32),
            pltpu.VMEM((lons, 2, cols), f32),
            pltpu.VMEM((owners, share, cols), f32),
            pltpu.VMEM((lons, share, cols), f32),
            pltpu.VMEM((rows // CORES * SUB, cols), f32),
            pltpu.VMEM((rows * SUB, cols), f32),
            pltpu.VMEM((SUB, cols), f32),
            pltpu.VMEM((SUB, cols), f32),
            dma((2,)),
            dma((3,)),
            dma,
        ]
        + [dma] * 11
        + [
            pltpu.SemaphoreType.REGULAR((2,)),
        ],
        compiler_params=pltpu.CompilerParams(
            collective_id=0, has_side_effects=True, vmem_limit_bytes=66879488
        ),
    )(
        flow.reshape(fields, rows, cols),
        warmth.reshape(fields, rows, cols),
        flag,
        floor,
        label,
    )
    eddy, transport = pl.pallas_call(
        write_out,
        out_shape=tuple(jax.ShapeDtypeStruct(a.shape, a.dtype) for a in (eddy, transport)),
        in_specs=[local] * 2,
        out_specs=[pl.BlockSpec(memory_space=pltpu.HBM)] * 2,
        scratch_shapes=[dma((2,))],
        compiler_params=pltpu.CompilerParams(vmem_limit_bytes=2**20),
    )(eddy, transport)
    return eddy, jnp.transpose(transport, (0, 3, 1, 2))


def solution(mesh):
    return jax.shard_map(
        functools.partial(shards, mesh.shape["lat"], mesh.shape["lon"]),
        mesh=mesh,
        in_specs=(
            P(None, None, "lat", "lon"),
            P(None, None, "lat", "lon"),
            P("lat", "lon"),
            P("lat", "lon"),
            P("lat", "lon"),
        ),
        out_specs=(P(None, "lat", "lon"), P(None, None, None, ("lat", "lon"))),
        check_vma=False,
    )
```

```python
import functools
import itertools
import math

import jax
import jax.numpy as jnp
from jax import lax
from jax.experimental import pallas as pl
from jax.experimental.pallas import tpu as pltpu
from jax.sharding import PartitionSpec as P

BASINS = 10
OWNER_PART = 8
CORES = 2
FAN = 4
GROUP = 16
SUB = 8
LANES = 128
MESH = pl.DeviceIdType.MESH


def kernel(
    dims,
    flow_hbm,
    warmth_hbm,
    flag_hbm,
    floor_hbm,
    label_hbm,
    eddy_ref,
    transport_ref,
    flow,
    warmth,
    flag,
    floor,
    label,
    depth,
    limit,
    mean_warmth,
    sums,
    split_even,
    split_odd,
    edge,
    edge_in,
    edge_sum,
    edge_sum_in,
    tiles,
    tiles_in,
    bar,
    bar_in,
    edge_line,
    edge_lines,
    lines,
    lines_in,
    tiles_near,
    tiles_last,
    last_tile,
    own_total,
    flow_sem,
    warmth_sem,
    small_sem,
    edge_send,
    edge_recv,
    edge_sum_recv,
    near_recv,
    tile_recv,
    bar_recv,
    line_recv,
    edge_line_send,
    edge_line_recv,
    sum_send,
    mean_send,
    met_sem,
):
    splits = (split_even, split_odd)
    times, levels, rows, pitch, lats, lons, owners, share, scaling = dims
    steps = rows // SUB
    lat, lon = lax.axis_index("lat"), lax.axis_index("lon")
    fields = times * levels
    last = rows - 1
    mine = pl.ds(pl.multiple_of(lon * SUB, SUB), SUB)
    places = round(math.log(lons, FAN))
    flat_flow = flow.reshape(fields * rows, LANES)
    flat_sums = sums.reshape(levels * pitch, LANES)
    flat_mean = mean_warmth.reshape(levels * rows, LANES)
    flat_warmth = warmth.reshape(fields * pitch, LANES)

    def flow_copy(n):
        part = pl.ds(pl.multiple_of(n * SUB, SUB), SUB)
        return pltpu.make_async_copy(flow_hbm.at[:, part], flow.at[:, part], flow_sem.at[2 * n // steps])

    def warmth_copy(n):
        part = pl.ds(pl.multiple_of(n * SUB, SUB), SUB)
        return pltpu.make_async_copy(warmth_hbm.at[:, part], warmth.at[:, part], warmth_sem.at[min(n, 1) + 2 * n // steps])

    smalls = [
        pltpu.make_async_copy(flag_hbm, flag, small_sem),
        pltpu.make_async_copy(floor_hbm, floor, small_sem),
        pltpu.make_async_copy(label_hbm, label, small_sem),
    ]

    def wait_rows(source, target, first, end, sem):
        part = pl.ds(first * SUB, (end - first) * SUB)
        pltpu.make_async_copy(source.at[:, part], target.at[:, part], sem).wait()

    warmth_copy(0).start()
    for copy in smalls:
        copy.start()

    barrier = pltpu.get_barrier_semaphore()
    turned_digits = [
        [lax.rem(lon // FAN**d + i, FAN) * FAN**d for i in range(FAN)] for d in range(places)
    ]
    reach = owners * CORES

    def owns(device):
        return (device < reach) & (lax.rem(device, CORES) == CORES - 1)

    is_owner = owns(lon)

    def far_first():
        ways = itertools.product(range(FAN), repeat=places)
        hops = lambda way: sum(min(i, FAN - i) for i in way[1:]) + (way[0] > 0)
        return [way for way in sorted(ways, key=hops, reverse=True) if any(way)]

    def at(way):
        return sum(turned_digits[d][way[d]] for d in range(places))

    def signal(semaphore, way):
        pl.semaphore_signal(semaphore, inc=1, device_id=(lat, at(way)), device_id_type=MESH)

    def line_ways(d):
        return [way for way in far_first() if way[d] and sum(i > 0 for i in way) == 1]

    @pl.when(is_owner)
    def _():
        for way in far_first():
            signal(barrier, way)

    @pl.when(jnp.logical_not(is_owner))
    def _():
        for way in far_first():
            if sum(i > 0 for i in way) == 1:
                signal(barrier, way)

    @pl.when(lat < lats - 1)
    def _():
        pl.semaphore_signal(barrier, inc=1, device_id=(lat + 1, lon), device_id_type=MESH)

    for n in range(1, steps):
        warmth_copy(n).start()
    for a in range(fields // SUB):
        flat_warmth[pl.ds(a * SUB * pitch + rows, SUB, stride=pitch), :] = jnp.zeros(
            (SUB, LANES), jnp.float32
        )
    for k in range(levels):
        flat_sums[k * pitch + rows : k * pitch + rows + SUB, :] = jnp.zeros(
            (SUB, LANES), jnp.float32
        )
    depth[rows : rows + SUB, :] = jnp.zeros((SUB, LANES), jnp.int32)
    own_chip = pl.ds(pl.multiple_of(lon // CORES * SUB, SUB), SUB)
    tiles_in[own_chip, :] = jnp.zeros((SUB, LANES), jnp.float32)
    pltpu.make_async_copy(
        flow_hbm.at[0 : len(smalls)], flow.at[0 : len(smalls)], small_sem
    ).wait()
    warmth_copy(0).wait()
    for n in range(steps):
        flow_copy(n).start()
    depth[0:rows, :] = flag[...] * floor[...]
    lane = lax.broadcasted_iota(jnp.int32, (SUB, LANES), 1)
    sub = lax.broadcasted_iota(jnp.int32, (SUB, LANES), 0)
    slots = times + 2
    turned = (lane + GROUP * sub) % LANES
    marks = [(turned >= BASINS * m) & (turned < BASINS * (m + 1)) for m in range(slots)]

    def two_parts(x):
        high = x.astype(jnp.bfloat16)
        return high, (x - high.astype(jnp.float32)).astype(jnp.bfloat16)

    def in_three(x):
        high = x.astype(jnp.bfloat16).astype(jnp.float32)
        rest = x - high
        middle = rest.astype(jnp.bfloat16).astype(jnp.float32)
        return [high, middle, rest - middle]

    def folded(out, size):
        return out[0:size, :] + out[size : 2 * size, :] + out[2 * size : 3 * size, :]

    def straight(x):
        return pltpu.roll(x, 0, axis=1, stride=GROUP, stride_axis=0)

    def hot_rows(n):
        iota = lax.broadcasted_iota(jnp.int32, (GROUP, LANES), 0)
        tags = label[n * SUB : (n + 1) * SUB, :]
        hot = jnp.concatenate(
            [
                jnp.where(
                    jnp.broadcast_to(tags[r : r + 1, :], (GROUP, LANES)) == iota, 1.0, 0.0
                )
                for r in (0, *range(SUB - 1, 0, -1))
            ],
            axis=0,
        ).astype(jnp.bfloat16)
        return jnp.concatenate([hot, hot], axis=1)

    def summed_over(data, hot):
        return lax.dot_general(
            data, hot, (((1,), (1,)), ((), ())), preferred_element_type=jnp.float32
        )

    def piece(out, c, m):
        x = out[c * SUB : (c + 1) * SUB, :]
        return pltpu.roll(x, BASINS * m, axis=1) if m else x

    def sum_times(n):
        here = pl.ds(n * SUB, SUB)
        for k in range(levels):
            sums[k, here, :] = functools.reduce(
                jnp.add, [warmth[t * levels + k, here, :] for t in range(times)]
            )

    wait_rows(warmth_hbm, warmth, 1, steps // 2, warmth_sem.at[1])
    for n in range(steps // 2):
        sum_times(n)
    wait_rows(warmth_hbm, warmth, steps // 2, steps, warmth_sem.at[2])
    for n in range(steps // 2, steps):
        sum_times(n)
    for n in range(steps):
        here = pl.ds(n * SUB, SUB)
        lim = jnp.minimum(depth[here, :], depth[pl.ds(n * SUB + 1, SUB), :])
        limit[here, :] = lim
        chunks = []
        for k in range(levels):
            wet = jnp.where(lim > k, 1.0, 0.0)
            mean_w = (sums[k, here, :] + flat_sums[pl.ds(k * pitch + n * SUB + 1, SUB), :]) * (
                0.5 / times
            )
            mean_warmth[k, here, :] = mean_w
            chunks += [wet, mean_w * wet]
        data = jnp.concatenate(in_three(jnp.concatenate(chunks, axis=0)), axis=0)
        out = summed_over(data.astype(jnp.bfloat16), hot_rows(n)[:, 0:LANES])
        out = folded(out, 2 * levels * SUB)
        line = jnp.zeros((SUB, LANES), jnp.float32)
        for k in range(levels):
            line = jnp.where(marks[k], piece(out, 2 * k, k), line)
            line = jnp.where(marks[levels + k], piece(out, 2 * k + 1, levels + k), line)
        line = straight(line)
        lines[n * SUB // share : (n + 1) * SUB // share] = line.reshape(
            SUB // share, share, LANES
        )

    edge_sum[...] = jnp.concatenate(
        [flat_sums[pl.ds(0, levels, stride=pitch), :], depth[0:levels, :].astype(jnp.float32)],
        axis=0,
    )
    edge_sum_copy = pltpu.make_async_remote_copy(
        src_ref=edge_sum,
        dst_ref=edge_sum_in,
        send_sem=edge_send,
        recv_sem=edge_sum_recv,
        device_id=(lat - 1, lon),
        device_id_type=MESH,
    )
    edge_copy = pltpu.make_async_remote_copy(
        src_ref=edge,
        dst_ref=edge_in,
        send_sem=edge_send,
        recv_sem=edge_recv,
        device_id=(lat - 1, lon),
        device_id_type=MESH,
    )
    plain = [
        jnp.where(owns(at(way)), 0, 1) for d in range(places) for way in line_ways(d)
    ]
    met = sum(plain) + owners - jnp.where(is_owner, 1, 0)
    pl.semaphore_wait(barrier, jnp.where(lat > 0, met + 1, met))

    @pl.when(lat > 0)
    def _():
        edge_sum_copy.start()

    for way in line_ways(1):
        signal(met_sem.at[0], way)

    def to_device(src, dst, send_sem, recv_sem, device):
        return pltpu.make_async_remote_copy(
            src_ref=src,
            dst_ref=dst,
            send_sem=send_sem,
            recv_sem=recv_sem,
            device_id=(lat, device),
            device_id_type=MESH,
        )

    inner = FAN ** (places - 1)
    for shift in sorted(range(FAN), key=lambda i: -min(i, FAN - i)):
        for rest in itertools.product(range(reach // inner), range(FAN // CORES)):
            owner = rest[0] * inner + turned_digits[1][shift] + rest[1] * CORES + CORES - 1

            def start(owner=owner):
                mine_there = lines_in.at[lon]
                to_device(
                    lines.at[owner // CORES], mine_there, mean_send, line_recv, owner
                ).start()

            if shift:
                start()
            else:
                pl.when(owner != lon)(start)

    @pl.when(is_owner)
    def _():
        lines_in[pl.ds(lon, 1)] = lines[pl.ds(lon // CORES, 1)]

    for a in range(fields // SUB):
        edge[a * SUB : (a + 1) * SUB, :] = flat_warmth[pl.ds(a * SUB * pitch, SUB, stride=pitch), :]

    @pl.when(lat > 0)
    def _():
        edge_copy.start()

    width = 2 * times + 4

    def prepare(n):
        row = n * SUB
        here = pl.ds(row, SUB)
        split = splits[n % 2]
        lim = limit[here, :]
        for k in range(levels):
            wet = jnp.where(lim > k, 1.0, 0.0)
            v = [flow[t * levels + k, here, :] for t in range(times)]
            w = [
                0.5
                * (
                    warmth[t * levels + k, here, :]
                    + flat_warmth[pl.ds((t * levels + k) * pitch + row + 1, SUB), :]
                )
                for t in range(times)
            ]
            mean_v = functools.reduce(jnp.add, v) * (1.0 / times)
            mean_w = mean_warmth[k, here, :]
            cross = functools.reduce(
                jnp.add, [(v[t] - mean_v) * (w[t] - mean_w) for t in range(times)]
            ) * (1.0 / times)
            chunks = [x * wet for x in v] + [x * wet for x in w]
            chunks += [wet, mean_v * mean_w * wet, cross * wet, jnp.zeros_like(wet)]
            for c in range(0, width, 2):
                high, low = two_parts(jnp.concatenate(chunks[c : c + 2], axis=0))
                at_row = (k * width + c) * SUB
                split[at_row : at_row + 2 * SUB, 0:LANES] = high
                split[at_row : at_row + 2 * SUB, LANES : 2 * LANES] = low

    def contract(n):
        out = summed_over(splits[n % 2][...], hot_rows(n))
        for k in range(levels):
            count = piece(out, k * width + 2 * times, times)
            for half in range(2):
                acc = jnp.where(marks[times], count, 0.0)
                for t in range(times):
                    acc = jnp.where(marks[t], piece(out, k * width + half * times + t, t), acc)
                both = piece(out, k * width + 2 * times + 1 + half, times + 1)
                acc = jnp.where(marks[times + 1], both, acc)
                tiles[pl.ds(n * SUB * SUB + half * levels + k, SUB, stride=SUB), :] = straight(acc)

    def last_hot(size):
        iota = lax.broadcasted_iota(jnp.int32, (size, LANES), 0)
        tags = jnp.broadcast_to(label[last : last + 1, :], (size, LANES))
        hot = jnp.where(tags == iota, 1.0, 0.0).astype(jnp.bfloat16)
        return jnp.concatenate([hot, hot], axis=1)

    def edge_line_of_sums():
        lim = jnp.minimum(
            depth[last : last + 1, :], edge_sum_in[levels : levels + 1, :].astype(jnp.int32)
        )
        limit[last : last + 1, :] = lim
        wet = jnp.where(jnp.broadcast_to(lim, (SUB, LANES)) > sub % levels, 1.0, 0.0)
        here = flat_sums[pl.ds(last, levels, stride=pitch), :]
        mean = (here + edge_sum_in[0:levels, :]) * (0.5 / times)
        flat_mean[pl.ds(last, levels, stride=rows), :] = mean
        chunk = wet * jnp.concatenate([jnp.ones_like(mean), mean], axis=0)
        data = jnp.concatenate([*in_three(chunk), jnp.zeros_like(chunk)], axis=0)
        iota = lax.broadcasted_iota(jnp.int32, (LANES, LANES), 0)
        tags = jnp.broadcast_to(label[last : last + 1, :], (LANES, LANES))
        inside = (iota >= levels * BASINS) & (iota < 2 * levels * BASINS)
        hot = jnp.where(inside & (tags == iota % BASINS), 1.0, 0.0).astype(jnp.bfloat16)
        out = folded(summed_over(data.astype(jnp.bfloat16), hot), SUB)
        out = jnp.where(lane // BASINS - levels == sub % levels, out, 0.0)
        for shift in (1, 2):
            out = out + pltpu.roll(out, shift, axis=0)
        return jnp.concatenate([out[levels - 1 : levels, :], out[2 * levels - 1 :, :]], axis=0)

    def edge_tile():
        lim = limit[last : last + 1, :]
        wet = jnp.where(jnp.broadcast_to(lim, (SUB, LANES)) > sub % levels, 1.0, 0.0)
        x = []
        for t in range(times):
            v = flat_flow[pl.ds(t * levels * rows + last, levels, stride=rows), :]
            w = flat_warmth[pl.ds(t * levels * pitch + last, levels, stride=pitch), :]
            w = 0.5 * (w + edge_in[t * levels : (t + 1) * levels, :])
            x.append(jnp.concatenate([v, w], axis=0))
        mean = functools.reduce(jnp.add, x) * (1.0 / times)
        devs = [y - mean for y in x]
        cross = functools.reduce(jnp.add, [y * other_half(y) for y in devs]) * (1.0 / times)
        both = jnp.where(sub < levels, mean * other_half(mean), cross)
        chunks = jnp.concatenate([y * wet for y in x] + [wet, both * wet], axis=0)
        data = jnp.concatenate(two_parts(chunks), axis=1)
        out = summed_over(data, last_hot(LANES))
        return functools.reduce(jnp.add, [piece(out, m, m) for m in range(slots)])

    def other_half(x):
        return pltpu.roll(x, levels, axis=0)

    def wait_for(ref, count, send_sem, recv_sem):
        part = pl.ds(0, count)
        return pltpu.make_async_remote_copy(
            src_ref=ref.at[part],
            dst_ref=ref.at[part],
            send_sem=send_sem,
            recv_sem=recv_sem,
            device_id=(lat, lon),
            device_id_type=MESH,
        )

    cuts = (0, steps // 2, steps)
    for low_cut, high_cut in itertools.pairwise(cuts):
        wait_rows(flow_hbm, flow, low_cut, high_cut, flow_sem.at[2 * low_cut // steps])
        for n in range(low_cut, high_cut):
            prepare(n)
            if n:
                contract(n - 1)
        if high_cut < steps:
            pl.semaphore_wait(met_sem.at[0], FAN - 1)
            for way in line_ways(places - 1):
                signal(met_sem.at[1], way)
    contract(steps - 1)
    core = lax.rem(lon, CORES)
    partner = lon + 1 - CORES * core

    def tile(ref, row):
        return ref.at[pl.ds(pl.multiple_of(row * SUB, SUB), SUB)]

    pairs = rows // CORES
    for i in range(pairs):
        to_device(
            tile(tiles, CORES * i + 1 - core), tile(tiles_near, i), sum_send, near_recv, partner
        ).start()

    every_line = wait_for(lines_in, lons - 1, mean_send, line_recv)
    every_bar = wait_for(bar_in, owners, mean_send, bar_recv)
    fewer_bars = wait_for(bar_in, owners - 1, mean_send, bar_recv)
    every_edge_line = wait_for(edge_lines, lons - 1, edge_line_send, edge_line_recv)
    every_near = wait_for(tiles_near, pairs * SUB, sum_send, near_recv)
    every_tile = wait_for(tiles_in, (pairs - 1) * SUB, sum_send, tile_recv)
    every_last = wait_for(tiles_last, (lons - 1) * SUB, sum_send, tile_recv)

    def tree_sum(parts):
        while len(parts) > 1:
            parts = [sum(parts[i : i + 2][1:], parts[i]) for i in range(0, len(parts), 2)]
        return parts[0]

    def ratio(total):
        return total / jnp.maximum(pltpu.roll(total, levels * BASINS, axis=1), 1.0)

    pl.semaphore_wait(met_sem.at[1], FAN - 1)

    every_near.wait_recv()
    for i in range(pairs):
        own = pl.ds(pl.multiple_of((CORES * i + core) * SUB, SUB), SUB)
        tiles[own, :] = tiles[own, :] + tiles_near[i * SUB : (i + 1) * SUB, :]
    for way in far_first():
        if way[0] % CORES == 0:
            peer = at(way)

            @pl.when(peer != last)
            def _():
                to_device(
                    tile(tiles, peer), tile(tiles_in, lon // CORES), sum_send, tile_recv, peer
                ).start()

    @pl.when(lat < lats - 1)
    def _():
        edge_sum_copy.wait_recv()

    @pl.when(lat == lats - 1)
    def _():
        edge_sum_in[...] = jnp.zeros_like(edge_sum_in)

    line = edge_line_of_sums()
    edge_line[...] = line
    edge_lines[pl.ds(lon, 1)] = line[None]
    for peer in map(at, far_first()):
        to_device(edge_line, edge_lines.at[lon], edge_line_send, edge_line_recv, peer).start()

    @pl.when(is_owner)
    def _():
        every_line.wait_recv()
        bar[...] = ratio(tree_sum([lines_in[p] for p in range(lons)]))
        bar_in[pl.ds(lon // CORES, 1)] = bar[...][None]
        for peer in map(at, far_first()):
            to_device(bar, bar_in.at[lon // CORES], mean_send, bar_recv, peer).start()

    @pl.when(lat < lats - 1)
    def _():
        edge_copy.wait_recv()

    @pl.when(lat == lats - 1)
    def _():
        edge_in[...] = jnp.zeros_like(edge_in)

    last_tile[...] = edge_tile()
    tiles_last[mine, :] = last_tile[...]

    @pl.when(lon != last)
    def _():
        to_device(last_tile, tile(tiles_last, lon), sum_send, tile_recv, last).start()

    def tiles_of(ref, count):
        return [ref[SUB * p : SUB * (p + 1), :] for p in range(count)]

    @pl.when(lon != last)
    def _():
        every_tile.wait_recv()
        own_total[...] = tree_sum([tiles[mine, :], *tiles_of(tiles_in, pairs)])

    @pl.when(lon == last)
    def _():
        every_last.wait_recv()
        own_total[...] = tree_sum(tiles_of(tiles_last, lons))

    total = own_total[...]

    def moved(x, lanes):
        return pltpu.roll(x, (-lanes) % LANES, axis=1)

    count = moved(total, BASINS * times)
    first = lane < BASINS
    divisor = jnp.maximum(count, 1.0)
    time_sums = total
    for t in range(1, times):
        time_sums = time_sums + moved(total, BASINS * t)
    bars = jnp.where(first, time_sums / divisor * (1.0 / times), 0.0)

    bars_w = other_half(bars)
    flow_part = scaling * count * bars * bars_w
    swing = jnp.zeros_like(total)
    for t in range(times):
        dev = (moved(total, 10 * t) if t else total) / divisor - bars
        swing = swing + dev * other_half(dev)
    swing = scaling * count * (swing * (1.0 / times))
    both = moved(total, 10 * (times + 1))
    steady = scaling * both - flow_part
    transient = scaling * other_half(both) - swing
    for q, value in enumerate((flow_part, steady, swing, transient)):
        for k in range(levels):
            transport_ref[q, k] = value[k : k + 1, 0:BASINS]

    every_edge_line.wait_recv()
    total = tree_sum([edge_lines[p] for p in range(lons)])
    last_bars = total[1:2, :] / jnp.maximum(total[0:1, :], 1.0)
    @pl.when(is_owner)
    def _():
        fewer_bars.wait_recv()

    @pl.when(jnp.logical_not(is_owner))
    def _():
        every_bar.wait_recv()

    for n in range(steps):
        here = slice(n * SUB, (n + 1) * SUB)
        table = bar_in[n * SUB // share : (n + 1) * SUB // share].reshape(SUB, LANES)
        if n == steps - 1:
            table = jnp.where(sub == SUB - 1, jnp.broadcast_to(last_bars, table.shape), table)
        lim = limit[here, :]
        tags = label[here, :]
        for k in range(levels):
            cell = jnp.take_along_axis(
                table, tags + (levels + k) * BASINS, axis=1, mode="promise_in_bounds"
            )
            eddy_ref[k, here, :] = jnp.where(lim > k, mean_warmth[k, here, :] - cell, 0.0)

    every_edge_line.wait_send()

    def wait_sent(count, semaphore):
        wait_for(flat_flow, count, semaphore, edge_recv).wait_send()

    @pl.when(core == CORES - 1)
    def _():
        wait_sent((2 * pairs - 1) * SUB, sum_send)

    @pl.when(core < CORES - 1)
    def _():
        wait_sent(2 * pairs * SUB, sum_send)

    @pl.when(is_owner)
    def _():
        wait_sent((owners - 1 + lons - 1) * share, mean_send)

    @pl.when(jnp.logical_not(is_owner))
    def _():
        wait_sent(owners * share, mean_send)

    @pl.when(lat > 0)
    def _():
        wait_sent(fields + 2 * levels, edge_send)


def write_out(eddy, transport, eddy_out, transport_out, sem):
    for k in range(eddy.shape[0]):
        pltpu.make_async_copy(eddy.at[k], eddy_out.at[k], sem.at[0]).start()
    small = pltpu.make_async_copy(transport, transport_out, sem.at[1])
    small.start()
    pltpu.make_async_copy(eddy, eddy_out, sem.at[0]).wait()
    small.wait()


def shards(lats, lons, flow, warmth, flag, floor, label):
    times, levels, rows, cols = flow.shape
    fields = times * levels
    pitch = rows + SUB
    scaling = 1.0 / math.sqrt(cols * lons)
    owners = lons // OWNER_PART
    share = rows // owners
    dims = (times, levels, rows, pitch, lats, lons, owners, share, scaling)
    local = pl.BlockSpec(memory_space=pltpu.VMEM)
    dma = pltpu.SemaphoreType.DMA
    f32 = jnp.float32
    eddy, transport = pl.pallas_call(
        functools.partial(kernel, dims),
        out_shape=(
            pltpu.VMEM((levels, rows, cols), f32),
            pltpu.VMEM((4, levels, 1, BASINS), f32),
        ),
        in_specs=[pl.BlockSpec(memory_space=pltpu.HBM)] * 5,
        out_specs=(local, local),
        scratch_shapes=[
            pltpu.VMEM((fields, rows, cols), f32),
            pltpu.VMEM((fields, pitch, cols), f32),
            pltpu.VMEM((rows, cols), jnp.int32),
            pltpu.VMEM((rows, cols), jnp.int32),
            pltpu.VMEM((rows, cols), jnp.int32),
            pltpu.VMEM((pitch, cols), jnp.int32),
            pltpu.VMEM((rows, cols), jnp.int32),
            pltpu.VMEM((levels, rows, cols), f32),
            pltpu.VMEM((levels, pitch, cols), f32),
            pltpu.VMEM((levels * (2 * times + 4) * SUB, 2 * cols), jnp.bfloat16),
            pltpu.VMEM((levels * (2 * times + 4) * SUB, 2 * cols), jnp.bfloat16),
            pltpu.VMEM((fields, cols), f32),
            pltpu.VMEM((fields, cols), f32),
            pltpu.VMEM((2 * levels, cols), f32),
            pltpu.VMEM((2 * levels, cols), f32),
            pltpu.VMEM((rows * SUB, cols), f32),
            pltpu.VMEM((rows // CORES * SUB, cols), f32),
            pltpu.VMEM((share, cols), f32),
            pltpu.VMEM((owners, share, cols), f32),
            pltpu.VMEM((2, cols), f32),
            pltpu.VMEM((lons, 2, cols), f32),
            pltpu.VMEM((owners, share, cols), f32),
            pltpu.VMEM((lons, share, cols), f32),
            pltpu.VMEM((rows // CORES * SUB, cols), f32),
            pltpu.VMEM((rows * SUB, cols), f32),
            pltpu.VMEM((SUB, cols), f32),
            pltpu.VMEM((SUB, cols), f32),
            dma((2,)),
            dma((3,)),
            dma,
        ]
        + [dma] * 11
        + [
            pltpu.SemaphoreType.REGULAR((2,)),
        ],
        compiler_params=pltpu.CompilerParams(
            collective_id=0, has_side_effects=True, vmem_limit_bytes=66879488
        ),
    )(
        flow.reshape(fields, rows, cols),
        warmth.reshape(fields, rows, cols),
        flag,
        floor,
        label,
    )
    eddy, transport = pl.pallas_call(
        write_out,
        out_shape=tuple(jax.ShapeDtypeStruct(a.shape, a.dtype) for a in (eddy, transport)),
        in_specs=[local] * 2,
        out_specs=[pl.BlockSpec(memory_space=pltpu.HBM)] * 2,
        scratch_shapes=[dma((2,))],
        compiler_params=pltpu.CompilerParams(vmem_limit_bytes=2**20),
    )(eddy, transport)
    return eddy, jnp.transpose(transport, (0, 3, 1, 2))


def solution(mesh):
    return jax.shard_map(
        functools.partial(shards, mesh.shape["lat"], mesh.shape["lon"]),
        mesh=mesh,
        in_specs=(
            P(None, None, "lat", "lon"),
            P(None, None, "lat", "lon"),
            P("lat", "lon"),
            P("lat", "lon"),
            P("lat", "lon"),
        ),
        out_specs=(P(None, "lat", "lon"), P(None, None, None, ("lat", "lon"))),
        check_vma=False,
    )
```
